32 devices in a mesh: dp: 4 (over y, x), rows: 2 (over core), cols: 4 (over z).
Axes of the slice: x: 2, y: 2, z: 4, core: 2. Of those that a mesh axis runs over, the one named last changes fastest.
Arguments:
- tokens: bfloat16 [4, 2, 1024, 768], P(None, 'rows', 'dp', 'cols'), may hold values from -6 to 6
- cotangent: bfloat16 [4, 2, 1024, 768], P(None, 'rows', 'dp', 'cols'), may hold values from -6 to 6
- labels: int32 [4, 2], P(None, 'rows'), may hold values from 0 to 13
- q_weight: bfloat16 [768, 768], P('rows', 'cols'), may hold values from -0.3125 to 0.3125
- k_weight: bfloat16 [768, 768], P('rows', 'cols'), may hold values from -0.3125 to 0.3125
- v_weight: bfloat16 [768, 768], P('rows', 'cols'), may hold values from -0.21875 to 0.21875
- out_weight: bfloat16 [768, 768], P('cols', 'rows'), may hold values from -2.5 to 2.5
- up_weight: bfloat16 [768, 3072], P('rows', 'cols'), may hold values from -0.21875 to 0.21875
- down_weight: bfloat16 [3072, 768], P('cols', 'rows'), may hold values from -0.109375 to 0.109375
- ln1_gain: float32 [768], P('cols'), may hold values from 0.5 to 1.5
- ln1_bias: float32 [768], P('cols'), may hold values from -3 to 3
- ln2_gain: float32 [768], P('cols'), may hold values from 0.5 to 1.5
- ln2_bias: float32 [768], P('cols'), may hold values from -3 to 3
- cls_in: bfloat16 [768, 128], P('cols'), may hold values from -0.21875 to 0.21875
- pool_query: float32 [2, 64], replicated, may hold values from -8 to 8
- cls_mid: float32 [128, 128], replicated, may hold values from -0.5 to 0.5
- cls_out: float32 [128, 14], replicated, may hold values from -1.5 to 1.5
Outputs:
- out_y: bfloat16 [4, 2, 1024, 768], P(None, 'rows', 'dp', 'cols')
- losses: float32 [4, 2], P(None, 'rows')
- grad_tokens: float32 [4, 2, 1024, 768], P(None, 'rows', 'dp', 'cols')
- grad_q_weight: float32 [768, 768], P('rows', 'cols')
- grad_k_weight: float32 [768, 768], P('rows', 'cols')
- grad_v_weight: float32 [768, 768], P('rows', 'cols')
- grad_out_weight: float32 [768, 768], P('cols', 'rows')
- grad_up_weight: float32 [768, 3072], P('rows', 'cols')
- grad_down_weight: float32 [3072, 768], P('cols', 'rows')
- grad_ln1_gain: float32 [768], P('cols')
- grad_ln1_bias: float32 [768], P('cols')
- grad_ln2_gain: float32 [768], P('cols')
- grad_ln2_bias: float32 [768], P('cols')
- grad_cls_in: float32 [768, 128], P('cols')
- grad_pool_query: float32 [2, 64], replicated
- grad_cls_mid: float32 [128, 128], replicated
- grad_cls_out: float32 [128, 14], replicated
The draws below stay inside these ranges and needn't reach their ends.
All inputs are finite; a program needn't handle non-finite values.
Results may differ from the reference program's by a relative error of at most 0.034.
Values may be sent and summed in bfloat16 or wider, within the bound.
A program may use at most 192 MiB of HBM per device.

```python
import math
import jax
import jax.numpy as jnp
from jax import lax

D = 768
HEADS = 12
FF = 3072
HDIM = 64
CLS_D = 128
POOL_HEADS = 2
CLASSES = 14
MICRO = 4
LEN = 1024
SEQS = 2


def set_ends(values, key, least, top_value):
    shape = values.shape
    index_at = [jax.random.randint(jax.random.fold_in(key, axis), (), 0, shape[axis]) for axis in range(len(shape))]
    values = values.at[tuple(index_at)].set(least)
    longest = shape.index(max(shape))
    index_at[longest] = (index_at[longest] + 1) % shape[longest]
    return values.at[tuple(index_at)].set(top_value)


def shard_levels(stream_key, dims, shards, smallest, top_value):
    def one(dim, blocks):
        draws = jax.random.uniform(jax.random.fold_in(jax.random.fold_in(stream_key, 6), dim), (blocks,), jnp.float32, smallest / len(shards), top_value / len(shards))
        return jnp.repeat(jnp.exp(draws), dims[dim] // blocks).reshape((-1,) + (1,) * (len(dims) - dim - 1))

    loudness = one(*shards[0])
    for cut in shards[1:]:
        loudness = loudness * one(*cut)
    return loudness


def bell_draw(key, extent, width, reach, split=(), dtype=jnp.bfloat16):
    values = jax.random.normal(key, extent, jnp.float32) * width
    if len(split) > 0:
        values = shard_levels(key, extent, split, -0.22, 0.18) * values
    return jnp.clip(values, min=-reach, max=reach).astype(dtype)


def setup_inputs(seed: int = 0) -> dict:
    key_list = jax.random.split(jax.random.key(seed), 18)
    tokens = bell_draw(key_list[0], (MICRO, SEQS, LEN, D), 1.0, 6.0, ((1, 2), (2, 4), (3, 4)))
    cotangent = bell_draw(key_list[1], (MICRO, SEQS, LEN, D), 1.0, 6.0, ((1, 2), (2, 4), (3, 4)))
    labels = set_ends(jax.random.randint(key_list[2], (MICRO, SEQS), 0, CLASSES), jax.random.fold_in(key_list[2], 1), 0, CLASSES - 1).astype(jnp.int32)
    q_weight = bell_draw(key_list[3], (D, D), (D // 2) ** -0.5, 0.3125, ((0, 2), (1, 4)))
    k_weight = bell_draw(key_list[4], (D, D), (D // 2) ** -0.5, 0.3125, ((0, 2), (1, 4)))
    v_weight = bell_draw(key_list[5], (D, D), D ** -0.5, 0.21875, ((0, 2), (1, 4)))
    out_weight = bell_draw(key_list[6], (D, D), (max(D // 128, 1)) ** -0.5, 2.5, ((0, 4), (1, 2)))
    up_weight = bell_draw(key_list[7], (D, FF), D ** -0.5, 0.21875, ((0, 2), (1, 4)))
    down_weight = bell_draw(key_list[8], (FF, D), FF ** -0.5, 0.109375, ((0, 4), (1, 2)))
    ln1_gain = jnp.clip(1.0 + 0.1 * jax.random.normal(key_list[9], (D,), jnp.float32), 0.5, 1.5)
    ln1_bias = bell_draw(key_list[10], (D,), 0.5, 3.0, ((0, 4),), jnp.float32)
    ln2_gain = jnp.clip(1.0 + 0.1 * jax.random.normal(key_list[11], (D,), jnp.float32), 0.5, 1.5)
    ln2_bias = bell_draw(key_list[12], (D,), 0.5, 3.0, ((0, 4),), jnp.float32)
    cls_in = bell_draw(key_list[13], (D, CLS_D), D ** -0.5, 0.21875, ((0, 4),))
    pool_query = bell_draw(key_list[14], (POOL_HEADS, CLS_D // POOL_HEADS), 2.0, 8.0, (), jnp.float32)
    cls_mid = bell_draw(key_list[15], (CLS_D, CLS_D), CLS_D ** -0.5, 0.5, (), jnp.float32)
    cls_out = bell_draw(key_list[16], (CLS_D, CLASSES), 0.25, 1.5, (), jnp.float32)
    return dict(tokens=tokens, cotangent=cotangent, labels=labels, q_weight=q_weight, k_weight=k_weight, v_weight=v_weight, out_weight=out_weight, up_weight=up_weight, down_weight=down_weight, ln1_gain=ln1_gain, ln1_bias=ln1_bias, ln2_gain=ln2_gain, ln2_bias=ln2_bias, cls_in=cls_in, pool_query=pool_query, cls_mid=cls_mid, cls_out=cls_out)


@jax.custom_vjp
def low(v):
    return lax.optimization_barrier(v.astype(jnp.bfloat16)).astype(jnp.float32)

@jax.custom_vjp
def low_back(v):
    return v

def low_keep(v):
    return (low(v), None)

def low_pass(kept, grad):
    return (grad,)

def back_keep(v):
    return (v, None)

def back_low(kept, grad):
    return (low(grad),)
low.defvjp(low_keep, low_pass)
low_back.defvjp(back_keep, back_low)
highest = lax.Precision.HIGHEST
eps_norm = 1e-12

def matmul(left_mat, right_mat):
    return jnp.dot(left_mat, right_mat, precision=highest, preferred_element_type=jnp.float32)

def layer_norm(hidden, gain_vec, shift_vec):
    average = lax.optimization_barrier(jnp.mean(hidden, axis=-1, keepdims=True))
    spread = lax.optimization_barrier(jnp.mean(hidden * hidden, axis=-1, keepdims=True)) - average * average
    return (hidden - average) * lax.rsqrt(spread + eps_norm) * gain_vec + shift_vec

def attention(queries, keys_all, values_all):
    length = queries.shape[0]
    query_heads = queries.reshape(length, HEADS, HDIM)
    key_heads = keys_all.reshape(length, HEADS, HDIM)
    value_heads = values_all.reshape(length, HEADS, HDIM)
    block_rows = math.gcd(length, 512)
    score_scale = 1.0 / math.sqrt(HDIM)

    def one_block(query_block):
        raw_scores = jnp.einsum('qhd,khd->hqk', query_block, key_heads, precision=highest)
        scores = low_back(raw_scores * score_scale)
        row_top = lax.optimization_barrier(jnp.max(scores, axis=-1, keepdims=True))
        exp_scores = jnp.exp(scores - row_top)
        softmaxed = exp_scores / lax.optimization_barrier(jnp.sum(exp_scores, axis=-1, keepdims=True))
        return jnp.einsum('hqk,khd->qhd', low(softmaxed), value_heads, precision=highest)
    blocks = query_heads.reshape(length // block_rows, block_rows, HEADS, HDIM)
    outputs = lax.map(jax.checkpoint(one_block), blocks)
    return outputs.reshape(length, D)

def forward(inputs, weight_set, class_label):
    q_weight, k_weight, v_weight, out_weight, up_weight, down_weight, ln1_gain, ln1_bias, ln2_gain, ln2_bias, cls_in, pool_query, cls_mid, cls_out = weight_set
    queries = low(low_back(matmul(inputs, q_weight)))
    keys_all = low(low_back(matmul(inputs, k_weight)))
    values_all = low(low_back(matmul(inputs, v_weight)))
    attended = low(low_back(attention(queries, keys_all, values_all)))
    branch = low_back(matmul(attended, out_weight))
    normed = layer_norm(inputs + branch, ln1_gain, ln1_bias)
    up_pre = low_back(matmul(low(normed), up_weight))
    activated = low(jax.nn.gelu(up_pre, approximate=False))
    down_out = low_back(matmul(activated, down_weight))
    outputs = layer_norm(normed + down_out, ln2_gain, ln2_bias)
    cls_proj = low_back(matmul(low(outputs), cls_in))
    length = cls_proj.shape[0]
    pool_dim = CLS_D // POOL_HEADS
    pool_heads = cls_proj.reshape(length, POOL_HEADS, pool_dim)
    pool_scores = jnp.einsum('lpd,pd->lp', pool_heads, pool_query, precision=highest) / math.sqrt(pool_dim)
    pool_weights = jax.nn.softmax(pool_scores, axis=0)
    pooled = jnp.einsum('lp,lpd->pd', pool_weights, pool_heads, precision=highest).reshape(1, CLS_D)
    hidden_cls = jnp.tanh(matmul(pooled, cls_mid))
    logits = matmul(hidden_cls, cls_out)[0]
    target_hit = lax.iota(jnp.int32, CLASSES) == class_label
    seq_loss = jax.nn.logsumexp(logits) - jnp.sum(jnp.where(target_hit, logits, 0.0))
    return (outputs, seq_loss)

def reference(tokens, cotangent, labels, q_weight, k_weight, v_weight, out_weight, up_weight, down_weight, ln1_gain, ln1_bias, ln2_gain, ln2_bias, cls_in, pool_query, cls_mid, cls_out):
    weight_set = tuple((entry.astype(jnp.float32) for entry in (q_weight, k_weight, v_weight, out_weight, up_weight, down_weight, ln1_gain, ln1_bias, ln2_gain, ln2_bias, cls_in, pool_query, cls_mid, cls_out)))
    seq_inputs = tokens.reshape(MICRO * SEQS, LEN, D).astype(jnp.float32)
    seq_cots = cotangent.reshape(MICRO * SEQS, LEN, D).astype(jnp.float32)
    seq_labels = labels.reshape(MICRO * SEQS)

    def one_sequence(totals, entry):
        inputs, upstream, class_label = entry

        def objective(inputs_now, weights_now):
            return forward(inputs_now, weights_now, class_label)
        (outputs, seq_loss), pullback = jax.vjp(objective, inputs, weight_set)
        grad_inputs, grad_weights = pullback((upstream, jnp.ones((), jnp.float32)))
        totals = tuple((left_val + right_val for left_val, right_val in zip(totals, grad_weights)))
        return (totals, (outputs.astype(jnp.bfloat16), seq_loss, grad_inputs))
    zeros = tuple((jnp.zeros_like(entry) for entry in weight_set))
    totals, (out_rows, loss_rows, grad_rows) = lax.scan(one_sequence, zeros, (seq_inputs, seq_cots, seq_labels))
    return (out_rows.reshape(MICRO, SEQS, LEN, D), loss_rows.reshape(MICRO, SEQS), grad_rows.reshape(MICRO, SEQS, LEN, D), totals[0], totals[1], totals[2], totals[3], totals[4], totals[5], totals[6], totals[7], totals[8], totals[9], totals[10], totals[11], totals[12], totals[13])
```

```python
import math

import jax
import jax.numpy as jnp
from jax import lax
from jax.experimental import pallas as pl
from jax.experimental.pallas import tpu as pltpu
from jax.sharding import PartitionSpec as P

MESH = pl.DeviceIdType.MESH
VMEM_GRANT = 60 * 1024 * 1024
HALF = 384


def split_rows(count):
    first = (count // 32) * 16 if (count // 2) % 16 else count // 2
    return (first, count - first)


def position():
    return (lax.axis_index("dp"), lax.axis_index("rows"), lax.axis_index("cols"))


def plane_x(p):
    return p + 1 - 2 * (p % 2)


def plane_y(p):
    return (p + 2) % 4


def greet(devices):
    barrier = pltpu.get_barrier_semaphore()
    for device in devices:
        pl.semaphore_signal(barrier, inc=1, device_id=device, device_id_type=MESH)
    pl.semaphore_wait(barrier, len(devices))


def remote(src, dst, send_sem, recv_sem, device):
    return pltpu.make_async_remote_copy(
        src_ref=src,
        dst_ref=dst,
        send_sem=send_sem,
        recv_sem=recv_sem,
        device_id=device,
        device_id_type=MESH,
    )


def comm_call(kernel, args, outs, scratch, ident):
    any_spec = pl.BlockSpec(memory_space=pl.ANY)
    return pl.pallas_call(
        kernel,
        out_shape=outs,
        in_specs=[any_spec] * len(args),
        out_specs=[any_spec] * len(outs),
        scratch_shapes=scratch,
        compiler_params=pltpu.CompilerParams(
            collective_id=ident, has_side_effects=True, vmem_limit_bytes=VMEM_GRANT
        ),
    )(*args)


def gather_kernel(swaps, casts, weights):
    def kernel(*refs):
        total = len(swaps) + len(casts) + len(weights)
        ins = refs[:total]
        outs = refs[total : 2 * total]
        zsend, zrecv, wsend, wrecv, local_sem = refs[2 * total :]
        p, r, c = position()
        px, py = plane_x(p), plane_y(p)
        others = [(p, r, (c + k) % 4) for k in range(1, 4)]
        twin = (p, 1 - r, c)
        greet(others + [(px, r, c), (py, r, c), twin])
        small = len(swaps) + len(casts)
        sent = []
        locals_ = []

        def keep(src, dst, index):
            copy = pltpu.make_async_copy(src, dst, local_sem.at[index])
            copy.start()
            locals_.append(copy)

        for index in range(small):
            for k in range(1, 4):
                peer = (c + k) % 4
                src = ins[index].at[peer] if index < len(swaps) else ins[index]
                copy = remote(
                    src,
                    outs[index].at[c],
                    zsend.at[index, k - 1],
                    zrecv.at[index, 3 - k],
                    (p, r, peer),
                )
                copy.start()
                sent.append(copy)
            keep(
                ins[index].at[c] if index < len(swaps) else ins[index], outs[index].at[c], index
            )

        lanes = pl.ds(pl.multiple_of(r * HALF, HALF), HALF)
        other_lanes = pl.ds(pl.multiple_of((1 - r) * HALF, HALF), HALF)

        def plan(g):
            src, dst = ins[small + g], outs[small + g]
            count = weights[g] // 4
            halves = split_rows(count)

            def rows(quarter, part=None):
                start = pl.multiple_of(quarter * count, 16)
                if part is None:
                    return pl.ds(start, count)
                return pl.ds(pl.multiple_of(start + part * halves[0], 16), halves[part])

            return src, dst, rows

        def z_sends(g):
            src, dst, rows = plan(g)
            copies = []
            for k in range(1, 4):
                peer = (c + k) % 4
                copy = remote(
                    src.at[rows(p)],
                    dst.at[c, rows(p), lanes],
                    wsend.at[g, k - 1],
                    wrecv.at[g, 3 - k],
                    (p, r, peer),
                )
                copy.start()
                copies.append(copy)
            copy = remote(src, dst.at[c, :, lanes], wsend.at[g, 3], wrecv.at[g, 3], twin)
            copy.start()
            copies.append(copy)
            keep(src, dst.at[c, :, lanes], small + g)
            return copies

        def forward(g, block, quarter, part, slot, device):
            _, dst, rows = plan(g)
            view = dst.at[block, rows(quarter, part), lanes]
            copy = remote(view, view, wsend.at[g, slot], wrecv.at[g, slot], device)
            copy.start()
            sent.append(copy)

        def arrived(g, block, quarter, part, slot, which):
            _, dst, rows = plan(g)
            view = dst.at[block, rows(quarter, part), which]
            remote(view, view, wsend.at[g, slot], wrecv.at[g, slot], twin).wait_recv()

        x_dev, y_dev = (px, r, c), (py, r, c)
        order = (1, 3, 2)
        diag = 3 - p

        def stage_plane(g):
            for k in order:
                block, base = (c + k) % 4, 4 + 9 * (k - 1)
                arrived(g, block, p, None, k - 1, lanes)
                forward(g, block, p, None, base, x_dev)
                forward(g, block, p, None, base + 1, y_dev)
                forward(g, block, p, None, base + 2, twin)

        def stage_relay(g):
            for k in order:
                block, base = (c + k) % 4, 4 + 9 * (k - 1)
                arrived(g, block, px, None, base, lanes)
                forward(g, block, px, 0, base + 3, y_dev)
                forward(g, block, px, None, base + 4, twin)
                arrived(g, block, py, None, base + 1, lanes)
                forward(g, block, py, 1, base + 5, x_dev)
                forward(g, block, py, None, base + 6, twin)

        def stage_last(g):
            for k in order:
                block, base = (c + k) % 4, 4 + 9 * (k - 1)
                arrived(g, block, diag, 0, base + 3, lanes)
                forward(g, block, diag, 0, base + 7, twin)
                arrived(g, block, diag, 1, base + 5, lanes)
                forward(g, block, diag, 1, base + 8, twin)

        count = len(weights)
        pending = z_sends(0)
        for step in range(count + 2):
            if step < count:
                for copy in pending:
                    copy.wait_send()
                if step + 1 < count:
                    pending = z_sends(step + 1)
                stage_plane(step)
            if 0 <= step - 1 < count:
                stage_relay(step - 1)
            if 0 <= step - 2 < count:
                stage_last(step - 2)

        for index in range(small):
            for k in range(1, 4):
                view = outs[index].at[(c + k) % 4]
                remote(view, view, zsend.at[index, k - 1], zrecv.at[index, k - 1], twin).wait_recv()
        for g in range(count):
            _, dst, rows = plan(g)
            view = dst.at[c, :, other_lanes]
            remote(view, view, wsend.at[g, 3], wrecv.at[g, 3], twin).wait_recv()
            for k in order:
                block, base = (c + k) % 4, 4 + 9 * (k - 1)
                arrived(g, block, p, None, base + 2, other_lanes)
                arrived(g, block, px, None, base + 4, other_lanes)
                arrived(g, block, py, None, base + 6, other_lanes)
                arrived(g, block, diag, 0, base + 7, other_lanes)
                arrived(g, block, diag, 1, base + 8, other_lanes)
        for copy in sent:
            copy.wait_send()
        for copy in locals_:
            copy.wait()

    return kernel


def gather_all(swaps, casts, weights):
    args = (*swaps, *casts, *weights)
    outs = [jax.ShapeDtypeStruct(a.shape, a.dtype) for a in swaps]
    outs += [jax.ShapeDtypeStruct((4,) + a.shape, a.dtype) for a in casts]
    outs += [jax.ShapeDtypeStruct((4, a.shape[0], 2 * HALF), a.dtype) for a in weights]
    small = len(swaps) + len(casts)
    dma = pltpu.SemaphoreType.DMA
    return comm_call(
        gather_kernel(swaps, casts, [a.shape[0] for a in weights]),
        args,
        outs,
        [
            dma((small, 3)),
            dma((small, 3)),
            dma((len(weights), 31)),
            dma((len(weights), 31)),
            dma((small + len(weights),)),
        ],
        1,
    )


def plane_kernel(number):
    def kernel(*refs):
        ins, outs = refs[:number], refs[number : 2 * number]
        send_sem, recv_sem, local_sem = refs[2 * number :]
        p, r, c = position()
        greet([((p + k) % 4, r, c) for k in range(1, 4)])
        copies, owns = [], []
        for index in range(number):
            for k in (2, 1, 3):
                peer = (p + k) % 4
                copy = remote(
                    ins[index].at[peer],
                    outs[index].at[p],
                    send_sem.at[index, k - 1],
                    recv_sem.at[index, 3 - k],
                    (peer, r, c),
                )
                copy.start()
                copies.append(copy)
            own = pltpu.make_async_copy(
                ins[index].at[p], outs[index].at[p], local_sem.at[index]
            )
            own.start()
            owns.append(own)
        for index in range(number):
            for k in range(1, 4):
                view = outs[index].at[(p + k) % 4]
                remote(
                    view, view, send_sem.at[index, k - 1], recv_sem.at[index, k - 1], (p, 1 - r, c)
                ).wait_recv()
        for copy in copies:
            copy.wait_send()
        for own in owns:
            own.wait()

    return kernel


def plane_swap(args, ident):
    dma = pltpu.SemaphoreType.DMA
    number = len(args)
    return comm_call(
        plane_kernel(number),
        args,
        [jax.ShapeDtypeStruct(a.shape, a.dtype) for a in args],
        [dma((number, 3)), dma((number, 3)), dma((number,))],
        ident,
    )


D = 768
HDIM = 64
CLS_D = 128
POOL_HEADS = 2
CLASSES = 14


eps_norm = 1e-12
highest = lax.Precision.HIGHEST


def merged(part, axis, combine):
    gathered = jax.tree.map(lambda a: lax.all_gather(a, axis), part)

    def take(source):
        return jax.tree.map(lambda a: lax.dynamic_index_in_dim(a, source, 0, False), gathered)

    return lax.fori_loop(
        1, lax.axis_size(axis), lambda source, state: combine(state, take(source)), take(0)
    )


def features(shard_part):
    return lax.all_gather(shard_part, "cols", axis=1, tiled=True)


def spread_sum(partial_value):
    return lax.psum_scatter(
        partial_value.astype(jnp.bfloat16), "cols", scatter_dimension=1, tiled=True
    ).astype(jnp.float32)


def token_sums(plain_sum, cross_sum):
    return lax.psum((plain_sum, cross_sum), "cols")


def dot_rows(left_mat, right_mat):
    return lax.dot_general(
        left_mat, right_mat, (((0,), (0,)), ((), ())), preferred_element_type=jnp.float32
    )


def dot_cols(left_mat, right_mat):
    return lax.dot_general(
        left_mat, right_mat, (((1,), (1,)), ((), ())), preferred_element_type=jnp.float32
    )


def exact_gelu(values):
    return jax.nn.gelu(values, approximate=False)


def norm_forward(hidden, gain_vec, shift_vec):
    plain_sum, squares = token_sums(jnp.sum(hidden, axis=1), jnp.sum(hidden * hidden, axis=1))
    average = plain_sum / D
    inv_std = lax.rsqrt(squares / D - average * average + eps_norm)
    centred = (hidden - average[:, None]) * inv_std[:, None]
    return (centred * gain_vec + shift_vec, centred, inv_std)


def norm_backward(upstream, centred, inv_std, gain_vec):
    scaled = upstream * gain_vec
    plain_sum, cross_sum = token_sums(jnp.sum(scaled, axis=1), jnp.sum(scaled * centred, axis=1))
    return inv_std[:, None] * (
        scaled - (plain_sum / D)[:, None] - centred * (cross_sum / D)[:, None]
    )


def block_size(number):
    return max((divisor for divisor in range(1, min(number, 1024) + 1) if number % divisor == 0))


def head_scores(query_heads, key_heads):
    return jnp.einsum(
        "qhd,khd->hqk", query_heads, key_heads, preferred_element_type=jnp.float32
    ) * (1.0 / math.sqrt(HDIM))


def split_pair(key_block, head_cols):
    block_rows = key_block.shape[0]
    key_heads = key_block[:, :head_cols].reshape(block_rows, head_cols // HDIM, HDIM)
    value_heads = key_block[:, head_cols:].reshape(block_rows, head_cols // HDIM, HDIM)
    return (key_heads, value_heads)


def fold_keys(running, shard_piece, query_heads):
    head_cols = query_heads.shape[1] * HDIM
    number = shard_piece.shape[0]
    block_rows = block_size(number)

    def fold_one_block(state_now, block_index):
        row_top, row_total, weighted = state_now
        key_block = lax.dynamic_slice_in_dim(shard_piece, block_index * block_rows, block_rows, 0)
        key_heads, value_heads = split_pair(key_block, head_cols)
        scores = head_scores(query_heads, key_heads)
        new_top = jnp.maximum(row_top, jnp.max(scores, axis=2))
        exp_scores = jnp.exp(scores - new_top[:, :, None])
        factor = jnp.exp(row_top - new_top)
        row_total = row_total * factor + jnp.sum(exp_scores, axis=2)
        weighted = weighted * jnp.transpose(factor)[:, :, None] + jnp.einsum(
            "hqk,khd->qhd",
            exp_scores.astype(jnp.bfloat16),
            value_heads,
            preferred_element_type=jnp.float32,
        )
        return ((new_top, row_total, weighted), None)

    running, unused = lax.scan(fold_one_block, running, jnp.arange(number // block_rows))
    return running


def score_grads(query_heads, key_heads, value_heads, grad_heads, log_total, delta_rows):
    softmaxed = jnp.exp(head_scores(query_heads, key_heads) - log_total[:, :, None])
    dprobs = jnp.einsum("qhd,khd->hqk", grad_heads, value_heads, preferred_element_type=jnp.float32)
    return (softmaxed, (softmaxed * (dprobs - delta_rows[:, :, None])).astype(jnp.bfloat16))


def joint_grads(pair_all, query_heads, grad_heads, log_total, delta_rows):
    head_cols = query_heads.shape[1] * HDIM
    number = pair_all.shape[0]
    block_rows = block_size(number)
    inv_root = 1.0 / math.sqrt(HDIM)

    def joint_one_block(accum, block_index):
        key_block = lax.dynamic_slice_in_dim(pair_all, block_index * block_rows, block_rows, 0)
        key_heads, value_heads = split_pair(key_block, head_cols)
        softmaxed, dscores = score_grads(
            query_heads, key_heads, value_heads, grad_heads, log_total, delta_rows
        )
        accum = accum + jnp.einsum(
            "hqk,khd->qhd", dscores, key_heads, preferred_element_type=jnp.float32
        )
        dkeys_block = (
            jnp.einsum("hqk,qhd->khd", dscores, query_heads, preferred_element_type=jnp.float32)
            * inv_root
        )
        dvalues = jnp.einsum(
            "hqk,qhd->khd",
            softmaxed.astype(jnp.bfloat16),
            grad_heads,
            preferred_element_type=jnp.float32,
        )
        return (
            accum,
            jnp.concatenate(
                [
                    dkeys_block.reshape(block_rows, head_cols),
                    dvalues.reshape(block_rows, head_cols),
                ],
                axis=1,
            ),
        )

    accum, blocks = lax.scan(
        joint_one_block, jnp.zeros(query_heads.shape, jnp.float32), jnp.arange(number // block_rows)
    )
    return (accum * inv_root, blocks.reshape(number, 2 * head_cols))


def pool_combine(left_part, right_part):
    top_left, total_left, sum_left = left_part
    top_right, total_right, sum_right = right_part
    joint_top = jnp.maximum(top_left, top_right)
    scale_left = jnp.exp(top_left - joint_top)
    scale_right = jnp.exp(top_right - joint_top)
    return (
        joint_top,
        total_left * scale_left + total_right * scale_right,
        sum_left * scale_left[:, None] + sum_right * scale_right[:, None],
    )


def reduce_weights(grad_set, head_cols):
    grad_qkv, grad_attn_out, grad_up, grad_down = grad_set
    part_q, part_k, part_v, part_out, part_up, part_down = (
        lax.psum_scatter(
            grad_qkv[:, :head_cols].astype(jnp.bfloat16), "rows", scatter_dimension=0, tiled=True
        ).astype(jnp.float32),
        lax.psum_scatter(
            grad_qkv[:, head_cols : 2 * head_cols].astype(jnp.bfloat16),
            "rows",
            scatter_dimension=0,
            tiled=True,
        ).astype(jnp.float32),
        lax.psum_scatter(
            grad_qkv[:, 2 * head_cols :].astype(jnp.bfloat16),
            "rows",
            scatter_dimension=0,
            tiled=True,
        ).astype(jnp.float32),
        lax.psum_scatter(
            grad_attn_out.astype(jnp.bfloat16), "rows", scatter_dimension=1, tiled=True
        ).astype(jnp.float32),
        lax.psum_scatter(
            grad_up.astype(jnp.bfloat16), "rows", scatter_dimension=0, tiled=True
        ).astype(jnp.float32),
        lax.psum_scatter(
            grad_down.astype(jnp.bfloat16), "rows", scatter_dimension=1, tiled=True
        ).astype(jnp.float32),
    )
    return (
        lax.psum(part_q.astype(jnp.bfloat16), "dp").astype(jnp.float32),
        lax.psum(part_k.astype(jnp.bfloat16), "dp").astype(jnp.float32),
        lax.psum(part_v.astype(jnp.bfloat16), "dp").astype(jnp.float32),
        lax.psum(part_out.astype(jnp.bfloat16), "dp").astype(jnp.float32),
        lax.psum(part_up.astype(jnp.bfloat16), "dp").astype(jnp.float32),
        lax.psum(part_down.astype(jnp.bfloat16), "dp").astype(jnp.float32),
    )


def body(
    tokens,
    cotangent,
    labels,
    q_weight,
    k_weight,
    v_weight,
    out_weight,
    up_weight,
    down_weight,
    ln1_gain,
    ln1_bias,
    ln2_gain,
    ln2_bias,
    cls_in,
    pool_query,
    cls_mid,
    cls_out,
):
    q_full, k_full, v_full, out_full, up_full, down_full = (
        lax.all_gather(q_weight, "rows", axis=0, tiled=True),
        lax.all_gather(k_weight, "rows", axis=0, tiled=True),
        lax.all_gather(v_weight, "rows", axis=0, tiled=True),
        lax.all_gather(out_weight, "rows", axis=1, tiled=True),
        lax.all_gather(up_weight, "rows", axis=0, tiled=True),
        lax.all_gather(down_weight, "rows", axis=1, tiled=True),
    )
    qkv_full = jnp.concatenate([q_full, k_full, v_full], axis=1)
    head_cols = q_weight.shape[1]
    heads_here = head_cols // HDIM
    row_count = tokens.shape[2]
    pool_dim = CLS_D // POOL_HEADS
    pool_root = math.sqrt(pool_dim)
    local_grads = (
        jnp.zeros(qkv_full.shape, jnp.float32),
        jnp.zeros(out_full.shape, jnp.float32),
        jnp.zeros(up_full.shape, jnp.float32),
        jnp.zeros(down_full.shape, jnp.float32),
    )
    gain_one = jnp.zeros(ln1_gain.shape, jnp.float32)
    bias_one = jnp.zeros(ln1_gain.shape, jnp.float32)
    gain_two = jnp.zeros(ln1_gain.shape, jnp.float32)
    bias_two = jnp.zeros(ln1_gain.shape, jnp.float32)
    grad_cls_in = jnp.zeros(cls_in.shape, jnp.float32)
    grad_pool = jnp.zeros(pool_query.shape, jnp.float32)
    grad_mid = jnp.zeros(cls_mid.shape, jnp.float32)
    grad_top = jnp.zeros(cls_out.shape, jnp.float32)
    out_list = []
    loss_list = []
    grad_list = []
    for micro_index in range(tokens.shape[0]):
        inputs_here = tokens[micro_index, 0]
        inputs_full = features(inputs_here)
        qkv_rows = jnp.dot(inputs_full, qkv_full, preferred_element_type=jnp.float32).astype(
            jnp.bfloat16
        )
        query_heads = qkv_rows[:, :head_cols].reshape(row_count, heads_here, HDIM)
        pair_here = qkv_rows[:, head_cols:]
        start_state = (
            jnp.full((heads_here, row_count), -1e30, jnp.float32),
            jnp.zeros((heads_here, row_count), jnp.float32),
            jnp.zeros((row_count, heads_here, HDIM), jnp.float32),
        )
        pair_all = lax.all_gather(pair_here, "dp", axis=0, tiled=True)
        row_top, row_total, weighted = fold_keys(start_state, pair_all, query_heads)
        log_total = row_top + jnp.log(row_total)
        attended = weighted / jnp.transpose(row_total)[:, :, None]
        attended_low = attended.reshape(row_count, head_cols).astype(jnp.bfloat16)
        branch = spread_sum(jnp.dot(attended_low, out_full, preferred_element_type=jnp.float32))
        normed, centred_one, inv_one = norm_forward(
            inputs_here.astype(jnp.float32) + branch, ln1_gain, ln1_bias
        )
        normed_full = features(normed.astype(jnp.bfloat16))
        up_pre = jnp.dot(normed_full, up_full, preferred_element_type=jnp.float32)
        activated, gelu_back = jax.vjp(exact_gelu, up_pre)
        activated_low = activated.astype(jnp.bfloat16)
        down_out = spread_sum(jnp.dot(activated_low, down_full, preferred_element_type=jnp.float32))
        outputs, centred_two, inv_two = norm_forward(normed + down_out, ln2_gain, ln2_bias)
        outputs_low = outputs.astype(jnp.bfloat16)
        out_list.append(outputs_low)
        cls_proj = lax.psum(
            jnp.dot(outputs_low, cls_in, preferred_element_type=jnp.float32).astype(jnp.bfloat16),
            "cols",
        ).astype(jnp.float32)
        pool_heads = cls_proj.reshape(row_count, POOL_HEADS, pool_dim)
        pool_scores = (
            jnp.einsum("lpd,pd->lp", pool_heads, pool_query, precision=highest) / pool_root
        )
        local_top = jnp.max(pool_scores, axis=0)
        pool_exp = jnp.exp(pool_scores - local_top)
        pool_top, pool_total, pool_sum = merged(
            (
                local_top,
                jnp.sum(pool_exp, axis=0),
                jnp.einsum("lp,lpd->pd", pool_exp, pool_heads, precision=highest),
            ),
            "dp",
            pool_combine,
        )
        pooled = pool_sum / pool_total[:, None]
        pool_weights = jnp.exp(pool_scores - pool_top) / pool_total
        pooled_row = pooled.reshape(1, CLS_D)
        hidden_cls = jnp.tanh(jnp.dot(pooled_row, cls_mid, precision=highest))
        logits = jnp.dot(hidden_cls, cls_out, precision=highest)[0]
        target_hit = lax.iota(jnp.int32, CLASSES) == labels[micro_index, 0]
        loss_list.append(jax.nn.logsumexp(logits) - jnp.sum(jnp.where(target_hit, logits, 0.0)))
        dlogits = jax.nn.softmax(logits) - target_hit.astype(jnp.float32)
        grad_top = grad_top + hidden_cls[0][:, None] * dlogits[None, :]
        dhidden = jnp.dot(cls_out, dlogits, precision=highest)
        dpre_tanh = dhidden * (1.0 - hidden_cls[0] * hidden_cls[0])
        grad_mid = grad_mid + pooled_row[0][:, None] * dpre_tanh[None, :]
        dpooled = jnp.dot(cls_mid, dpre_tanh, precision=highest).reshape(POOL_HEADS, pool_dim)
        dweights = jnp.einsum("lpd,pd->lp", pool_heads, dpooled, precision=highest)
        centre_term = jnp.sum(pooled * dpooled, axis=1)
        dpool_scores = pool_weights * (dweights - centre_term)
        dheads = (
            pool_weights[:, :, None] * dpooled[None]
            + dpool_scores[:, :, None] * (pool_query / pool_root)[None]
        )
        grad_pool = (
            grad_pool
            + jnp.einsum("lp,lpd->pd", dpool_scores, pool_heads, precision=highest) / pool_root
        )
        dproj_low = dheads.reshape(row_count, CLS_D).astype(jnp.bfloat16)
        grad_cls_in = grad_cls_in + dot_rows(outputs_low, dproj_low)
        upstream = cotangent[micro_index, 0].astype(jnp.float32) + dot_cols(dproj_low, cls_in)
        gain_two = gain_two + jnp.sum(upstream * centred_two, axis=0)
        bias_two = bias_two + jnp.sum(upstream, axis=0)
        dhidden_two = norm_backward(upstream, centred_two, inv_two, ln2_gain)
        ddown_full = features(dhidden_two.astype(jnp.bfloat16))
        grad_down_now = dot_rows(activated_low, ddown_full)
        dact_grad = dot_cols(ddown_full, down_full)
        dup_low = gelu_back(dact_grad)[0].astype(jnp.bfloat16)
        grad_up_now = dot_rows(normed_full, dup_low)
        dnormed = dhidden_two + spread_sum(dot_cols(dup_low, up_full))
        gain_one = gain_one + jnp.sum(dnormed * centred_one, axis=0)
        bias_one = bias_one + jnp.sum(dnormed, axis=0)
        dhidden_one = norm_backward(dnormed, centred_one, inv_one, ln1_gain)
        dattn_full = features(dhidden_one.astype(jnp.bfloat16))
        grad_attn_now = dot_rows(attended_low, dattn_full)
        dattended = dot_cols(dattn_full, out_full).astype(jnp.bfloat16)
        grad_heads = dattended.reshape(row_count, heads_here, HDIM)
        delta_rows = jnp.transpose(jnp.sum(grad_heads.astype(jnp.float32) * attended, axis=2))
        dquery, pair_terms = joint_grads(pair_all, query_heads, grad_heads, log_total, delta_rows)
        dpair_sum = lax.psum_scatter(
            pair_terms.astype(jnp.bfloat16), "dp", scatter_dimension=0, tiled=True
        ).astype(jnp.float32)
        dqkv_low = jnp.concatenate(
            [dquery.reshape(row_count, head_cols), dpair_sum], axis=1
        ).astype(jnp.bfloat16)
        grad_qkv_now = dot_rows(inputs_full, dqkv_low)
        grad_list.append(dhidden_one + spread_sum(dot_cols(dqkv_low, qkv_full)))
        micro_grads = (grad_qkv_now, grad_attn_now, grad_up_now, grad_down_now)
        local_grads = tuple(
            (left_val + right_val for left_val, right_val in zip(local_grads, micro_grads))
        )
    final_set = reduce_weights(local_grads, head_cols)
    lead_mask = (lax.axis_index("dp") == 0).astype(jnp.float32)
    sum_gain1, sum_bias1, sum_gain2, sum_bias2, sum_cls_in, sum_pool, sum_mid, sum_top = lax.psum(
        (
            gain_one,
            bias_one,
            gain_two,
            bias_two,
            grad_cls_in,
            grad_pool,
            grad_mid * lead_mask,
            grad_top * lead_mask,
        ),
        ("dp", "rows"),
    )
    return (
        jnp.stack(out_list)[:, None],
        jnp.stack(loss_list)[:, None],
        jnp.stack(grad_list)[:, None],
        final_set[0],
        final_set[1],
        final_set[2],
        final_set[3],
        final_set[4],
        final_set[5],
        sum_gain1,
        sum_bias1,
        sum_gain2,
        sum_bias2,
        sum_cls_in,
        sum_pool,
        sum_mid,
        sum_top,
    )


def dot_at(left, right, contract):
    return lax.dot_general(
        left, right, (contract, ((), ())), preferred_element_type=jnp.float32
    )


NN = ((1,), (0,))
NT = ((1,), (1,))
TN = ((0,), (0,))


def wide(ref):
    return jnp.concatenate([ref[block] for block in range(ref.shape[0])], axis=1)


def attend_kernel(q_ref, k_ref, v_ref, o_ref, low_ref, p_ref, inv_ref):
    keys = wide(k_ref)
    values = wide(v_ref)
    for block in range(q_ref.shape[0]):
        query = q_ref[block]
        scores = dot_at(keys, query, TN) * 0.125
        exps = jnp.exp(scores - jnp.max(scores, axis=0, keepdims=True))
        inverse = 1.0 / jnp.sum(exps, axis=0, keepdims=True)
        low = exps.astype(jnp.bfloat16)
        p_ref[0, block] = low
        inv_ref[0, block] = inverse
        out = dot_at(values, low, NN) * inverse
        o_ref[block] = out
        low_ref[block] = out.astype(jnp.bfloat16)


def attend(qkv):
    blocks, _, width = qkv.shape
    heads = qkv.shape[1] // 192

    def part(offset):
        return pl.BlockSpec((blocks, 64, width), lambda h: (0, h + offset * heads, 0))

    total = blocks * width
    return pl.pallas_call(
        attend_kernel,
        grid=(heads,),
        out_shape=[
            jax.ShapeDtypeStruct((blocks, 64 * heads, width), jnp.float32),
            jax.ShapeDtypeStruct((blocks, 64 * heads, width), jnp.bfloat16),
            jax.ShapeDtypeStruct((heads, blocks, total, width), jnp.bfloat16),
            jax.ShapeDtypeStruct((heads, blocks, 1, width), jnp.float32),
        ],
        in_specs=[part(0), part(1), part(2)],
        out_specs=[
            part(0),
            part(0),
            pl.BlockSpec((1, blocks, total, width), lambda h: (h, 0, 0, 0)),
            pl.BlockSpec((1, blocks, 1, width), lambda h: (h, 0, 0, 0)),
        ],
        compiler_params=pltpu.CompilerParams(vmem_limit_bytes=VMEM_GRANT),
    )(qkv, qkv, qkv)


def attend_back_kernel(q_ref, k_ref, v_ref, d_ref, o_ref, p_ref, inv_ref, dq_ref, dk_ref, dv_ref):
    keys = wide(k_ref)
    values = wide(v_ref)
    width = q_ref.shape[2]
    dkeys = jnp.zeros(keys.shape, jnp.float32)
    dvalues = jnp.zeros(keys.shape, jnp.float32)
    for block in range(q_ref.shape[0]):
        query = q_ref[block]
        grad = d_ref[block].astype(jnp.float32)
        inverse = inv_ref[0, block]
        delta = jnp.sum(grad * o_ref[block], axis=0, keepdims=True) * inverse
        scaled = (grad * inverse).astype(jnp.bfloat16)
        low = p_ref[0, block]
        dprobs = dot_at(values, scaled, TN)
        dscores = (low.astype(jnp.float32) * (dprobs - delta)).astype(jnp.bfloat16)
        dq_ref[block] = (dot_at(keys, dscores, NN) * 0.125).astype(jnp.bfloat16)
        dkeys = dkeys + dot_at(query, dscores, NT)
        dvalues = dvalues + dot_at(scaled, low, NT)
    for block in range(q_ref.shape[0]):
        span = slice(block * width, (block + 1) * width)
        dk_ref[block] = (dkeys[:, span] * 0.125).astype(jnp.bfloat16)
        dv_ref[block] = dvalues[:, span].astype(jnp.bfloat16)


def attend_back(qkv, grad, out, probs, inverse):
    blocks, _, width = qkv.shape
    heads = qkv.shape[1] // 192

    def part(offset):
        return pl.BlockSpec((blocks, 64, width), lambda h: (0, h + offset * heads, 0))

    total = blocks * width
    piece = jax.ShapeDtypeStruct((blocks, 64 * heads, width), jnp.bfloat16)
    return pl.pallas_call(
        attend_back_kernel,
        grid=(heads,),
        out_shape=[piece, piece, piece],
        in_specs=[
            part(0),
            part(1),
            part(2),
            part(0),
            part(0),
            pl.BlockSpec((1, blocks, total, width), lambda h: (h, 0, 0, 0)),
            pl.BlockSpec((1, blocks, 1, width), lambda h: (h, 0, 0, 0)),
        ],
        out_specs=[part(0), part(0), part(0)],
        compiler_params=pltpu.CompilerParams(vmem_limit_bytes=VMEM_GRANT),
    )(qkv, qkv, qkv, grad, out, probs, inverse)


def pool_exchange(part):
    return plane_swap((jnp.broadcast_to(part[None], (4,) + part.shape),), 3)[0]


def layer_norm_rows(hidden, gain_vec, shift_vec):
    average = jnp.mean(hidden, axis=1, keepdims=True)
    spread = jnp.mean(hidden * hidden, axis=1, keepdims=True) - average * average
    inv_std = lax.rsqrt(spread + eps_norm)
    centred = (hidden - average) * inv_std
    return (centred * gain_vec + shift_vec, centred, inv_std)


def layer_norm_back(upstream, centred, inv_std, gain_vec):
    scaled = upstream * gain_vec
    return inv_std * (
        scaled
        - jnp.mean(scaled, axis=1, keepdims=True)
        - centred * jnp.mean(scaled * centred, axis=1, keepdims=True)
    )


def quad_body(
    tokens,
    cotangent,
    labels,
    q_weight,
    k_weight,
    v_weight,
    out_weight,
    up_weight,
    down_weight,
    ln1_gain,
    ln1_bias,
    ln2_gain,
    ln2_bias,
    cls_in,
    pool_query,
    cls_mid,
    cls_out,
):
    low = jnp.bfloat16
    rows_here = tokens.shape[2]
    pool_dim = CLS_D // POOL_HEADS
    pool_root = math.sqrt(pool_dim)
    qkv_shard = jnp.concatenate([q_weight.T, k_weight.T, v_weight.T], axis=0)
    norm_shard = jnp.pad(
        jnp.stack([ln1_gain, ln1_bias, ln2_gain, ln2_bias]), ((0, 4), (0, 64))
    )
    x4, cot4, norms4, cls4, w_qkv, w_out, w_up, w_down = gather_all(
        (tokens[:, 0], cotangent[:, 0]),
        (norm_shard, cls_in),
        (qkv_shard, out_weight, up_weight.T, down_weight),
    )
    inputs = jnp.transpose(x4, (1, 0, 2)).reshape(rows_here, D)
    cot = jnp.transpose(cot4, (1, 0, 2)).reshape(rows_here, D)
    norms = jnp.transpose(norms4[:, :4, :192], (1, 0, 2)).reshape(4, D)
    gain_one, bias_one, gain_two, bias_two = (norms[i][None] for i in range(4))
    cls_full = cls4.reshape(D, CLS_D)
    w_qkv, w_out, w_up, w_down = (w.reshape(-1, D) for w in (w_qkv, w_out, w_up, w_down))

    qkv = dot_at(w_qkv, inputs, NT).astype(low).reshape(4, 576, rows_here)
    qkv = plane_swap((qkv,), 2)[0]
    attended, attended_heads, probs, inverse = attend(qkv)
    attended_low = plane_swap((attended_heads,), 4)[0].reshape(D, rows_here)
    branch = dot_at(attended_low, w_out, TN)
    normed, centred_one, inv_one = layer_norm_rows(
        inputs.astype(jnp.float32) + branch, gain_one, bias_one
    )
    normed_low = normed.astype(low)
    up_pre = dot_at(w_up, normed_low, NT)
    activated, gelu_back = jax.vjp(exact_gelu, up_pre)
    activated_low = activated.astype(low)
    down_out = dot_at(activated_low, w_down, TN)
    outputs, centred_two, inv_two = layer_norm_rows(normed + down_out, gain_two, bias_two)
    outputs_low = outputs.astype(low)
    cls_proj = jnp.dot(outputs_low, cls_full, preferred_element_type=jnp.float32)
    pool_heads = cls_proj.reshape(rows_here, POOL_HEADS, pool_dim)
    pool_scores = jnp.einsum("lpd,pd->lp", pool_heads, pool_query, precision=highest) / pool_root
    local_top = jnp.max(pool_scores, axis=0)
    pool_exp = jnp.exp(pool_scores - local_top)
    stats = jnp.stack(
        [
            jnp.repeat(local_top, pool_dim),
            jnp.repeat(jnp.sum(pool_exp, axis=0), pool_dim),
            jnp.einsum("lp,lpd->pd", pool_exp, pool_heads, precision=highest).reshape(CLS_D),
        ]
    )
    stats = pool_exchange(jnp.pad(stats, ((0, 5), (0, 0))))
    joint_top = jnp.max(stats[:, 0], axis=0)
    rescale = jnp.exp(stats[:, 0] - joint_top)
    joint_total = jnp.sum(stats[:, 1] * rescale, axis=0)
    pooled_row = (jnp.sum(stats[:, 2] * rescale, axis=0) / joint_total)[None]
    pooled = pooled_row.reshape(POOL_HEADS, pool_dim)
    pool_weights = jnp.exp(pool_scores - joint_top[::pool_dim]) / joint_total[::pool_dim]
    hidden_cls = jnp.tanh(jnp.dot(pooled_row, cls_mid, precision=highest))
    logits = jnp.dot(hidden_cls, cls_out, precision=highest)[0]
    col = lax.axis_index("cols")
    label = lax.dynamic_index_in_dim(labels[:, 0], col, 0, False)
    target_hit = lax.iota(jnp.int32, CLASSES) == label
    loss = jax.nn.logsumexp(logits) - jnp.sum(jnp.where(target_hit, logits, 0.0))
    dlogits = jax.nn.softmax(logits) - target_hit.astype(jnp.float32)
    grad_top = hidden_cls[0][:, None] * dlogits[None, :]
    dhidden = jnp.dot(cls_out, dlogits, precision=highest)
    dpre_tanh = dhidden * (1.0 - hidden_cls[0] * hidden_cls[0])
    grad_mid = pooled_row[0][:, None] * dpre_tanh[None, :]
    dpooled = jnp.dot(cls_mid, dpre_tanh, precision=highest).reshape(POOL_HEADS, pool_dim)
    dweights = jnp.einsum("lpd,pd->lp", pool_heads, dpooled, precision=highest)
    dpool_scores = pool_weights * (dweights - jnp.sum(pooled * dpooled, axis=1))
    dheads = (
        pool_weights[:, :, None] * dpooled[None]
        + dpool_scores[:, :, None] * (pool_query / pool_root)[None]
    )
    grad_pool = jnp.einsum("lp,lpd->pd", dpool_scores, pool_heads, precision=highest) / pool_root
    dproj_low = dheads.reshape(rows_here, CLS_D).astype(low)
    grad_cls_in = dot_rows(outputs_low, dproj_low)
    upstream = cot.astype(jnp.float32) + dot_cols(dproj_low, cls_full)
    sums = [jnp.sum(upstream * centred_two, axis=0), jnp.sum(upstream, axis=0)]
    dhidden_two = layer_norm_back(upstream, centred_two, inv_two, gain_two)
    ddown = dhidden_two.astype(low)
    g_down = dot_at(activated_low, ddown, NN).astype(low)
    dup = gelu_back(dot_at(w_down, ddown, NT))[0].astype(low)
    g_up = dot_at(dup, normed_low, NN).astype(low)
    dnormed = dhidden_two + dot_at(dup, w_up, TN)
    sums += [jnp.sum(dnormed * centred_one, axis=0), jnp.sum(dnormed, axis=0)]
    dhidden_one = layer_norm_back(dnormed, centred_one, inv_one, gain_one)
    dbranch = dhidden_one.astype(low)
    g_out = dot_at(attended_low, dbranch, NN).astype(low)
    dattended = dot_at(w_out, dbranch, NT).astype(low).reshape(4, 192, rows_here)
    dattended = plane_swap((dattended,), 5)[0]
    dqkv = jnp.concatenate(attend_back(qkv, dattended, attended, probs, inverse), axis=1)
    dqkv = plane_swap((dqkv,), 6)[0].reshape(4 * 576, rows_here)
    g_qkv = dot_at(dqkv, inputs, NN).astype(low)
    grad_inputs = dhidden_one + dot_at(dqkv, w_qkv, TN)

    lead = (lax.axis_index("dp") == 0).astype(jnp.float32)
    slot = lax.axis_index("rows") * 4 + col
    loss_row = jnp.where(lax.iota(jnp.int32, CLS_D) == slot, loss * lead, 0.0)
    packed = jnp.concatenate(
        [
            grad_cls_in,
            jnp.stack(sums).reshape(4 * D // CLS_D, CLS_D),
            grad_mid * lead,
            grad_top.T * lead,
            grad_pool.reshape(1, CLS_D),
            loss_row[None],
        ],
        axis=0,
    )
    packed = lax.psum(packed, ("dp", "rows", "cols"))
    sum_cls_in = lax.dynamic_slice_in_dim(packed[:D], col * 192, 192, 0)
    norm_sums = lax.dynamic_slice_in_dim(packed[D : D + 24].reshape(4, D), col * 192, 192, 1)
    at = D + 24
    sum_mid = packed[at : at + CLS_D]
    sum_top = packed[at + CLS_D : at + CLS_D + CLASSES].T
    sum_pool = packed[at + CLS_D + CLASSES].reshape(POOL_HEADS, pool_dim)
    losses = lax.dynamic_slice_in_dim(packed[at + CLS_D + CLASSES + 1], (slot - col), 4, 0)

    def features_out(value):
        blocks = jnp.transpose(value.reshape(rows_here, 4, 192), (1, 0, 2))
        return blocks

    out_blocks, grad_blocks, r_qkv, r_out, r_up, r_down = reduce_all(
        (features_out(outputs_low), features_out(grad_inputs.astype(low))),
        (g_qkv, g_out, g_up, g_down),
    )
    wide_ = jnp.float32
    return (
        out_blocks[:, None],
        losses[:, None],
        grad_blocks.astype(wide_)[:, None],
        r_qkv[:192].T.astype(wide_),
        r_qkv[192:384].T.astype(wide_),
        r_qkv[384:].T.astype(wide_),
        r_out.astype(wide_),
        r_up.T.astype(wide_),
        r_down.astype(wide_),
        norm_sums[2],
        norm_sums[3],
        norm_sums[0],
        norm_sums[1],
        sum_cls_in,
        sum_pool,
        sum_mid,
        sum_top,
    )


def reduce_all(swaps, grads):
    moved = [lax.all_to_all(a, "cols", 0, 0, tiled=True) for a in swaps]
    done = []
    for grad in grads:
        part = lax.psum_scatter(grad, "rows", scatter_dimension=1, tiled=True)
        part = lax.psum_scatter(part, "cols", scatter_dimension=0, tiled=True)
        done.append(lax.psum(part, "dp"))
    return (*moved, *done)


def solution(mesh):
    placed = (
        P(None, "rows", "dp", "cols"),
        P(None, "rows", "dp", "cols"),
        P(None, "rows"),
        P("rows", "cols"),
        P("rows", "cols"),
        P("rows", "cols"),
        P("cols", "rows"),
        P("rows", "cols"),
        P("cols", "rows"),
        P("cols"),
        P("cols"),
        P("cols"),
        P("cols"),
        P("cols", None),
        P(),
        P(),
        P(),
    )
    even = dict(mesh.shape) == {"dp": 4, "rows": 2, "cols": 4}
    return jax.shard_map(
        quad_body if even else body,
        mesh=mesh,
        in_specs=placed,
        out_specs=(
            P(None, "rows", "dp", "cols"),
            P(None, "rows"),
            P(None, "rows", "dp", "cols"),
            P("rows", "cols"),
            P("rows", "cols"),
            P("rows", "cols"),
            P("cols", "rows"),
            P("rows", "cols"),
            P("cols", "rows"),
            P("cols"),
            P("cols"),
            P("cols"),
            P("cols"),
            P("cols", None),
            P(),
            P(),
            P(),
        ),
        check_vma=False,
    )
```

```python
import math

import jax
import jax.numpy as jnp
from jax import lax
from jax.experimental import pallas as pl
from jax.experimental.pallas import tpu as pltpu
from jax.sharding import PartitionSpec as P

MESH = pl.DeviceIdType.MESH
VMEM_GRANT = 60 * 1024 * 1024
HALF = 384


def split_rows(count):
    first = (count // 32) * 16 if (count // 2) % 16 else count // 2
    return (first, count - first)


def position():
    return (lax.axis_index("dp"), lax.axis_index("rows"), lax.axis_index("cols"))


def plane_x(p):
    return p + 1 - 2 * (p % 2)


def plane_y(p):
    return (p + 2) % 4


def greet(devices):
    barrier = pltpu.get_barrier_semaphore()
    for device in devices:
        pl.semaphore_signal(barrier, inc=1, device_id=device, device_id_type=MESH)
    pl.semaphore_wait(barrier, len(devices))


def remote(src, dst, send_sem, recv_sem, device):
    return pltpu.make_async_remote_copy(
        src_ref=src,
        dst_ref=dst,
        send_sem=send_sem,
        recv_sem=recv_sem,
        device_id=device,
        device_id_type=MESH,
    )


def comm_call(kernel, args, outs, scratch, ident):
    any_spec = pl.BlockSpec(memory_space=pl.ANY)
    return pl.pallas_call(
        kernel,
        out_shape=outs,
        in_specs=[any_spec] * len(args),
        out_specs=[any_spec] * len(outs),
        scratch_shapes=scratch,
        compiler_params=pltpu.CompilerParams(
            collective_id=ident, has_side_effects=True, vmem_limit_bytes=VMEM_GRANT
        ),
    )(*args)


def gather_kernel(swaps, casts, weights):
    def kernel(*refs):
        total = len(swaps) + len(casts) + len(weights)
        ins = refs[:total]
        outs = refs[total : 2 * total]
        zsend, zrecv, wsend, wrecv, local_sem = refs[2 * total :]
        p, r, c = position()
        px, py = plane_x(p), plane_y(p)
        others = [(p, r, (c + k) % 4) for k in range(1, 4)]
        twin = (p, 1 - r, c)
        greet(others + [(px, r, c), (py, r, c), twin])
        small = len(swaps) + len(casts)
        sent = []
        locals_ = []

        def keep(src, dst, index):
            copy = pltpu.make_async_copy(src, dst, local_sem.at[index])
            copy.start()
            locals_.append(copy)

        for index in range(small):
            for k in range(1, 4):
                peer = (c + k) % 4
                src = ins[index].at[peer] if index < len(swaps) else ins[index]
                copy = remote(
                    src,
                    outs[index].at[c],
                    zsend.at[index, k - 1],
                    zrecv.at[index, 3 - k],
                    (p, r, peer),
                )
                copy.start()
                sent.append(copy)
            keep(
                ins[index].at[c] if index < len(swaps) else ins[index], outs[index].at[c], index
            )

        lanes = pl.ds(pl.multiple_of(r * HALF, HALF), HALF)
        other_lanes = pl.ds(pl.multiple_of((1 - r) * HALF, HALF), HALF)

        def plan(g):
            src, dst = ins[small + g], outs[small + g]
            count = weights[g] // 4
            halves = split_rows(count)

            def rows(quarter, part=None):
                start = pl.multiple_of(quarter * count, 16)
                if part is None:
                    return pl.ds(start, count)
                return pl.ds(pl.multiple_of(start + part * halves[0], 16), halves[part])

            return src, dst, rows

        def z_sends(g):
            src, dst, rows = plan(g)
            copies = []
            for k in range(1, 4):
                peer = (c + k) % 4
                copy = remote(
                    src.at[rows(p)],
                    dst.at[c, rows(p), lanes],
                    wsend.at[g, k - 1],
                    wrecv.at[g, 3 - k],
                    (p, r, peer),
                )
                copy.start()
                copies.append(copy)
            copy = remote(src, dst.at[c, :, lanes], wsend.at[g, 3], wrecv.at[g, 3], twin)
            copy.start()
            copies.append(copy)
            keep(src, dst.at[c, :, lanes], small + g)
            return copies

        def forward(g, block, quarter, part, slot, device):
            _, dst, rows = plan(g)
            view = dst.at[block, rows(quarter, part), lanes]
            copy = remote(view, view, wsend.at[g, slot], wrecv.at[g, slot], device)
            copy.start()
            sent.append(copy)

        def arrived(g, block, quarter, part, slot, which):
            _, dst, rows = plan(g)
            view = dst.at[block, rows(quarter, part), which]
            remote(view, view, wsend.at[g, slot], wrecv.at[g, slot], twin).wait_recv()

        x_dev, y_dev = (px, r, c), (py, r, c)
        order = (1, 3, 2)
        diag = 3 - p

        def stage_plane(g):
            for k in order:
                block, base = (c + k) % 4, 4 + 9 * (k - 1)
                arrived(g, block, p, None, k - 1, lanes)
                forward(g, block, p, None, base, x_dev)
                forward(g, block, p, None, base + 1, y_dev)
                forward(g, block, p, None, base + 2, twin)

        def stage_relay(g):
            for k in order:
                block, base = (c + k) % 4, 4 + 9 * (k - 1)
                arrived(g, block, px, None, base, lanes)
                forward(g, block, px, 0, base + 3, y_dev)
                forward(g, block, px, None, base + 4, twin)
                arrived(g, block, py, None, base + 1, lanes)
                forward(g, block, py, 1, base + 5, x_dev)
                forward(g, block, py, None, base + 6, twin)

        def stage_last(g):
            for k in order:
                block, base = (c + k) % 4, 4 + 9 * (k - 1)
                arrived(g, block, diag, 0, base + 3, lanes)
                forward(g, block, diag, 0, base + 7, twin)
                arrived(g, block, diag, 1, base + 5, lanes)
                forward(g, block, diag, 1, base + 8, twin)

        count = len(weights)
        pending = z_sends(0)
        for step in range(count + 2):
            if step < count:
                for copy in pending:
                    copy.wait_send()
                if step + 1 < count:
                    pending = z_sends(step + 1)
                stage_plane(step)
            if 0 <= step - 1 < count:
                stage_relay(step - 1)
            if 0 <= step - 2 < count:
                stage_last(step - 2)

        for index in range(small):
            for k in range(1, 4):
                view = outs[index].at[(c + k) % 4]
                remote(view, view, zsend.at[index, k - 1], zrecv.at[index, k - 1], twin).wait_recv()
        for g in range(count):
            _, dst, rows = plan(g)
            view = dst.at[c, :, other_lanes]
            remote(view, view, wsend.at[g, 3], wrecv.at[g, 3], twin).wait_recv()
            for k in order:
                block, base = (c + k) % 4, 4 + 9 * (k - 1)
                arrived(g, block, p, None, base + 2, other_lanes)
                arrived(g, block, px, None, base + 4, other_lanes)
                arrived(g, block, py, None, base + 6, other_lanes)
                arrived(g, block, diag, 0, base + 7, other_lanes)
                arrived(g, block, diag, 1, base + 8, other_lanes)
        for copy in sent:
            copy.wait_send()
        for copy in locals_:
            copy.wait()

    return kernel


def gather_all(swaps, casts, weights):
    args = (*swaps, *casts, *weights)
    outs = [jax.ShapeDtypeStruct(a.shape, a.dtype) for a in swaps]
    outs += [jax.ShapeDtypeStruct((4,) + a.shape, a.dtype) for a in casts]
    outs += [jax.ShapeDtypeStruct((4, a.shape[0], 2 * HALF), a.dtype) for a in weights]
    small = len(swaps) + len(casts)
    dma = pltpu.SemaphoreType.DMA
    return comm_call(
        gather_kernel(swaps, casts, [a.shape[0] for a in weights]),
        args,
        outs,
        [
            dma((small, 3)),
            dma((small, 3)),
            dma((len(weights), 31)),
            dma((len(weights), 31)),
            dma((small + len(weights),)),
        ],
        1,
    )


def plane_kernel(number):
    def kernel(*refs):
        ins, outs = refs[:number], refs[number : 2 * number]
        send_sem, recv_sem, local_sem = refs[2 * number :]
        p, r, c = position()
        greet([((p + k) % 4, r, c) for k in range(1, 4)])
        copies, owns = [], []
        for index in range(number):
            for k in (2, 1, 3):
                peer = (p + k) % 4
                copy = remote(
                    ins[index].at[peer],
                    outs[index].at[p],
                    send_sem.at[index, k - 1],
                    recv_sem.at[index, 3 - k],
                    (peer, r, c),
                )
                copy.start()
                copies.append(copy)
            own = pltpu.make_async_copy(
                ins[index].at[p], outs[index].at[p], local_sem.at[index]
            )
            own.start()
            owns.append(own)
        for index in range(number):
            for k in range(1, 4):
                view = outs[index].at[(p + k) % 4]
                remote(
                    view, view, send_sem.at[index, k - 1], recv_sem.at[index, k - 1], (p, 1 - r, c)
                ).wait_recv()
        for copy in copies:
            copy.wait_send()
        for own in owns:
            own.wait()

    return kernel


def plane_swap(args, ident):
    dma = pltpu.SemaphoreType.DMA
    number = len(args)
    return comm_call(
        plane_kernel(number),
        args,
        [jax.ShapeDtypeStruct(a.shape, a.dtype) for a in args],
        [dma((number, 3)), dma((number, 3)), dma((number,))],
        ident,
    )


D = 768
HDIM = 64
CLS_D = 128
POOL_HEADS = 2
CLASSES = 14


eps_norm = 1e-12
highest = lax.Precision.HIGHEST


def merged(part, axis, combine):
    gathered = jax.tree.map(lambda a: lax.all_gather(a, axis), part)

    def take(source):
        return jax.tree.map(lambda a: lax.dynamic_index_in_dim(a, source, 0, False), gathered)

    return lax.fori_loop(
        1, lax.axis_size(axis), lambda source, state: combine(state, take(source)), take(0)
    )


def features(shard_part):
    return lax.all_gather(shard_part, "cols", axis=1, tiled=True)


def spread_sum(partial_value):
    return lax.psum_scatter(
        partial_value.astype(jnp.bfloat16), "cols", scatter_dimension=1, tiled=True
    ).astype(jnp.float32)


def token_sums(plain_sum, cross_sum):
    return lax.psum((plain_sum, cross_sum), "cols")


def dot_rows(left_mat, right_mat):
    return lax.dot_general(
        left_mat, right_mat, (((0,), (0,)), ((), ())), preferred_element_type=jnp.float32
    )


def dot_cols(left_mat, right_mat):
    return lax.dot_general(
        left_mat, right_mat, (((1,), (1,)), ((), ())), preferred_element_type=jnp.float32
    )


def exact_gelu(values):
    return jax.nn.gelu(values, approximate=False)


def norm_forward(hidden, gain_vec, shift_vec):
    plain_sum, squares = token_sums(jnp.sum(hidden, axis=1), jnp.sum(hidden * hidden, axis=1))
    average = plain_sum / D
    inv_std = lax.rsqrt(squares / D - average * average + eps_norm)
    centred = (hidden - average[:, None]) * inv_std[:, None]
    return (centred * gain_vec + shift_vec, centred, inv_std)


def norm_backward(upstream, centred, inv_std, gain_vec):
    scaled = upstream * gain_vec
    plain_sum, cross_sum = token_sums(jnp.sum(scaled, axis=1), jnp.sum(scaled * centred, axis=1))
    return inv_std[:, None] * (
        scaled - (plain_sum / D)[:, None] - centred * (cross_sum / D)[:, None]
    )


def block_size(number):
    return max((divisor for divisor in range(1, min(number, 1024) + 1) if number % divisor == 0))


def head_scores(query_heads, key_heads):
    return jnp.einsum(
        "qhd,khd->hqk", query_heads, key_heads, preferred_element_type=jnp.float32
    ) * (1.0 / math.sqrt(HDIM))


def split_pair(key_block, head_cols):
    block_rows = key_block.shape[0]
    key_heads = key_block[:, :head_cols].reshape(block_rows, head_cols // HDIM, HDIM)
    value_heads = key_block[:, head_cols:].reshape(block_rows, head_cols // HDIM, HDIM)
    return (key_heads, value_heads)


def fold_keys(running, shard_piece, query_heads):
    head_cols = query_heads.shape[1] * HDIM
    number = shard_piece.shape[0]
    block_rows = block_size(number)

    def fold_one_block(state_now, block_index):
        row_top, row_total, weighted = state_now
        key_block = lax.dynamic_slice_in_dim(shard_piece, block_index * block_rows, block_rows, 0)
        key_heads, value_heads = split_pair(key_block, head_cols)
        scores = head_scores(query_heads, key_heads)
        new_top = jnp.maximum(row_top, jnp.max(scores, axis=2))
        exp_scores = jnp.exp(scores - new_top[:, :, None])
        factor = jnp.exp(row_top - new_top)
        row_total = row_total * factor + jnp.sum(exp_scores, axis=2)
        weighted = weighted * jnp.transpose(factor)[:, :, None] + jnp.einsum(
            "hqk,khd->qhd",
            exp_scores.astype(jnp.bfloat16),
            value_heads,
            preferred_element_type=jnp.float32,
        )
        return ((new_top, row_total, weighted), None)

    running, unused = lax.scan(fold_one_block, running, jnp.arange(number // block_rows))
    return running


def score_grads(query_heads, key_heads, value_heads, grad_heads, log_total, delta_rows):
    softmaxed = jnp.exp(head_scores(query_heads, key_heads) - log_total[:, :, None])
    dprobs = jnp.einsum("qhd,khd->hqk", grad_heads, value_heads, preferred_element_type=jnp.float32)
    return (softmaxed, (softmaxed * (dprobs - delta_rows[:, :, None])).astype(jnp.bfloat16))


def joint_grads(pair_all, query_heads, grad_heads, log_total, delta_rows):
    head_cols = query_heads.shape[1] * HDIM
    number = pair_all.shape[0]
    block_rows = block_size(number)
    inv_root = 1.0 / math.sqrt(HDIM)

    def joint_one_block(accum, block_index):
        key_block = lax.dynamic_slice_in_dim(pair_all, block_index * block_rows, block_rows, 0)
        key_heads, value_heads = split_pair(key_block, head_cols)
        softmaxed, dscores = score_grads(
            query_heads, key_heads, value_heads, grad_heads, log_total, delta_rows
        )
        accum = accum + jnp.einsum(
            "hqk,khd->qhd", dscores, key_heads, preferred_element_type=jnp.float32
        )
        dkeys_block = (
            jnp.einsum("hqk,qhd->khd", dscores, query_heads, preferred_element_type=jnp.float32)
            * inv_root
        )
        dvalues = jnp.einsum(
            "hqk,qhd->khd",
            softmaxed.astype(jnp.bfloat16),
            grad_heads,
            preferred_element_type=jnp.float32,
        )
        return (
            accum,
            jnp.concatenate(
                [
                    dkeys_block.reshape(block_rows, head_cols),
                    dvalues.reshape(block_rows, head_cols),
                ],
                axis=1,
            ),
        )

    accum, blocks = lax.scan(
        joint_one_block, jnp.zeros(query_heads.shape, jnp.float32), jnp.arange(number // block_rows)
    )
    return (accum * inv_root, blocks.reshape(number, 2 * head_cols))


def pool_combine(left_part, right_part):
    top_left, total_left, sum_left = left_part
    top_right, total_right, sum_right = right_part
    joint_top = jnp.maximum(top_left, top_right)
    scale_left = jnp.exp(top_left - joint_top)
    scale_right = jnp.exp(top_right - joint_top)
    return (
        joint_top,
        total_left * scale_left + total_right * scale_right,
        sum_left * scale_left[:, None] + sum_right * scale_right[:, None],
    )


def reduce_weights(grad_set, head_cols):
    grad_qkv, grad_attn_out, grad_up, grad_down = grad_set
    part_q, part_k, part_v, part_out, part_up, part_down = (
        lax.psum_scatter(
            grad_qkv[:, :head_cols].astype(jnp.bfloat16), "rows", scatter_dimension=0, tiled=True
        ).astype(jnp.float32),
        lax.psum_scatter(
            grad_qkv[:, head_cols : 2 * head_cols].astype(jnp.bfloat16),
            "rows",
            scatter_dimension=0,
            tiled=True,
        ).astype(jnp.float32),
        lax.psum_scatter(
            grad_qkv[:, 2 * head_cols :].astype(jnp.bfloat16),
            "rows",
            scatter_dimension=0,
            tiled=True,
        ).astype(jnp.float32),
        lax.psum_scatter(
            grad_attn_out.astype(jnp.bfloat16), "rows", scatter_dimension=1, tiled=True
        ).astype(jnp.float32),
        lax.psum_scatter(
            grad_up.astype(jnp.bfloat16), "rows", scatter_dimension=0, tiled=True
        ).astype(jnp.float32),
        lax.psum_scatter(
            grad_down.astype(jnp.bfloat16), "rows", scatter_dimension=1, tiled=True
        ).astype(jnp.float32),
    )
    return (
        lax.psum(part_q.astype(jnp.bfloat16), "dp").astype(jnp.float32),
        lax.psum(part_k.astype(jnp.bfloat16), "dp").astype(jnp.float32),
        lax.psum(part_v.astype(jnp.bfloat16), "dp").astype(jnp.float32),
        lax.psum(part_out.astype(jnp.bfloat16), "dp").astype(jnp.float32),
        lax.psum(part_up.astype(jnp.bfloat16), "dp").astype(jnp.float32),
        lax.psum(part_down.astype(jnp.bfloat16), "dp").astype(jnp.float32),
    )


def body(
    tokens,
    cotangent,
    labels,
    q_weight,
    k_weight,
    v_weight,
    out_weight,
    up_weight,
    down_weight,
    ln1_gain,
    ln1_bias,
    ln2_gain,
    ln2_bias,
    cls_in,
    pool_query,
    cls_mid,
    cls_out,
):
    q_full, k_full, v_full, out_full, up_full, down_full = (
        lax.all_gather(q_weight, "rows", axis=0, tiled=True),
        lax.all_gather(k_weight, "rows", axis=0, tiled=True),
        lax.all_gather(v_weight, "rows", axis=0, tiled=True),
        lax.all_gather(out_weight, "rows", axis=1, tiled=True),
        lax.all_gather(up_weight, "rows", axis=0, tiled=True),
        lax.all_gather(down_weight, "rows", axis=1, tiled=True),
    )
    qkv_full = jnp.concatenate([q_full, k_full, v_full], axis=1)
    head_cols = q_weight.shape[1]
    heads_here = head_cols // HDIM
    row_count = tokens.shape[2]
    pool_dim = CLS_D // POOL_HEADS
    pool_root = math.sqrt(pool_dim)
    local_grads = (
        jnp.zeros(qkv_full.shape, jnp.float32),
        jnp.zeros(out_full.shape, jnp.float32),
        jnp.zeros(up_full.shape, jnp.float32),
        jnp.zeros(down_full.shape, jnp.float32),
    )
    gain_one = jnp.zeros(ln1_gain.shape, jnp.float32)
    bias_one = jnp.zeros(ln1_gain.shape, jnp.float32)
    gain_two = jnp.zeros(ln1_gain.shape, jnp.float32)
    bias_two = jnp.zeros(ln1_gain.shape, jnp.float32)
    grad_cls_in = jnp.zeros(cls_in.shape, jnp.float32)
    grad_pool = jnp.zeros(pool_query.shape, jnp.float32)
    grad_mid = jnp.zeros(cls_mid.shape, jnp.float32)
    grad_top = jnp.zeros(cls_out.shape, jnp.float32)
    out_list = []
    loss_list = []
    grad_list = []
    for micro_index in range(tokens.shape[0]):
        inputs_here = tokens[micro_index, 0]
        inputs_full = features(inputs_here)
        qkv_rows = jnp.dot(inputs_full, qkv_full, preferred_element_type=jnp.float32).astype(
            jnp.bfloat16
        )
        query_heads = qkv_rows[:, :head_cols].reshape(row_count, heads_here, HDIM)
        pair_here = qkv_rows[:, head_cols:]
        start_state = (
            jnp.full((heads_here, row_count), -1e30, jnp.float32),
            jnp.zeros((heads_here, row_count), jnp.float32),
            jnp.zeros((row_count, heads_here, HDIM), jnp.float32),
        )
        pair_all = lax.all_gather(pair_here, "dp", axis=0, tiled=True)
        row_top, row_total, weighted = fold_keys(start_state, pair_all, query_heads)
        log_total = row_top + jnp.log(row_total)
        attended = weighted / jnp.transpose(row_total)[:, :, None]
        attended_low = attended.reshape(row_count, head_cols).astype(jnp.bfloat16)
        branch = spread_sum(jnp.dot(attended_low, out_full, preferred_element_type=jnp.float32))
        normed, centred_one, inv_one = norm_forward(
            inputs_here.astype(jnp.float32) + branch, ln1_gain, ln1_bias
        )
        normed_full = features(normed.astype(jnp.bfloat16))
        up_pre = jnp.dot(normed_full, up_full, preferred_element_type=jnp.float32)
        activated, gelu_back = jax.vjp(exact_gelu, up_pre)
        activated_low = activated.astype(jnp.bfloat16)
        down_out = spread_sum(jnp.dot(activated_low, down_full, preferred_element_type=jnp.float32))
        outputs, centred_two, inv_two = norm_forward(normed + down_out, ln2_gain, ln2_bias)
        outputs_low = outputs.astype(jnp.bfloat16)
        out_list.append(outputs_low)
        cls_proj = lax.psum(
            jnp.dot(outputs_low, cls_in, preferred_element_type=jnp.float32).astype(jnp.bfloat16),
            "cols",
        ).astype(jnp.float32)
        pool_heads = cls_proj.reshape(row_count, POOL_HEADS, pool_dim)
        pool_scores = (
            jnp.einsum("lpd,pd->lp", pool_heads, pool_query, precision=highest) / pool_root
        )
        local_top = jnp.max(pool_scores, axis=0)
        pool_exp = jnp.exp(pool_scores - local_top)
        pool_top, pool_total, pool_sum = merged(
            (
                local_top,
                jnp.sum(pool_exp, axis=0),
                jnp.einsum("lp,lpd->pd", pool_exp, pool_heads, precision=highest),
            ),
            "dp",
            pool_combine,
        )
        pooled = pool_sum / pool_total[:, None]
        pool_weights = jnp.exp(pool_scores - pool_top) / pool_total
        pooled_row = pooled.reshape(1, CLS_D)
        hidden_cls = jnp.tanh(jnp.dot(pooled_row, cls_mid, precision=highest))
        logits = jnp.dot(hidden_cls, cls_out, precision=highest)[0]
        target_hit = lax.iota(jnp.int32, CLASSES) == labels[micro_index, 0]
        loss_list.append(jax.nn.logsumexp(logits) - jnp.sum(jnp.where(target_hit, logits, 0.0)))
        dlogits = jax.nn.softmax(logits) - target_hit.astype(jnp.float32)
        grad_top = grad_top + hidden_cls[0][:, None] * dlogits[None, :]
        dhidden = jnp.dot(cls_out, dlogits, precision=highest)
        dpre_tanh = dhidden * (1.0 - hidden_cls[0] * hidden_cls[0])
        grad_mid = grad_mid + pooled_row[0][:, None] * dpre_tanh[None, :]
        dpooled = jnp.dot(cls_mid, dpre_tanh, precision=highest).reshape(POOL_HEADS, pool_dim)
        dweights = jnp.einsum("lpd,pd->lp", pool_heads, dpooled, precision=highest)
        centre_term = jnp.sum(pooled * dpooled, axis=1)
        dpool_scores = pool_weights * (dweights - centre_term)
        dheads = (
            pool_weights[:, :, None] * dpooled[None]
            + dpool_scores[:, :, None] * (pool_query / pool_root)[None]
        )
        grad_pool = (
            grad_pool
            + jnp.einsum("lp,lpd->pd", dpool_scores, pool_heads, precision=highest) / pool_root
        )
        dproj_low = dheads.reshape(row_count, CLS_D).astype(jnp.bfloat16)
        grad_cls_in = grad_cls_in + dot_rows(outputs_low, dproj_low)
        upstream = cotangent[micro_index, 0].astype(jnp.float32) + dot_cols(dproj_low, cls_in)
        gain_two = gain_two + jnp.sum(upstream * centred_two, axis=0)
        bias_two = bias_two + jnp.sum(upstream, axis=0)
        dhidden_two = norm_backward(upstream, centred_two, inv_two, ln2_gain)
        ddown_full = features(dhidden_two.astype(jnp.bfloat16))
        grad_down_now = dot_rows(activated_low, ddown_full)
        dact_grad = dot_cols(ddown_full, down_full)
        dup_low = gelu_back(dact_grad)[0].astype(jnp.bfloat16)
        grad_up_now = dot_rows(normed_full, dup_low)
        dnormed = dhidden_two + spread_sum(dot_cols(dup_low, up_full))
        gain_one = gain_one + jnp.sum(dnormed * centred_one, axis=0)
        bias_one = bias_one + jnp.sum(dnormed, axis=0)
        dhidden_one = norm_backward(dnormed, centred_one, inv_one, ln1_gain)
        dattn_full = features(dhidden_one.astype(jnp.bfloat16))
        grad_attn_now = dot_rows(attended_low, dattn_full)
        dattended = dot_cols(dattn_full, out_full).astype(jnp.bfloat16)
        grad_heads = dattended.reshape(row_count, heads_here, HDIM)
        delta_rows = jnp.transpose(jnp.sum(grad_heads.astype(jnp.float32) * attended, axis=2))
        dquery, pair_terms = joint_grads(pair_all, query_heads, grad_heads, log_total, delta_rows)
        dpair_sum = lax.psum_scatter(
            pair_terms.astype(jnp.bfloat16), "dp", scatter_dimension=0, tiled=True
        ).astype(jnp.float32)
        dqkv_low = jnp.concatenate(
            [dquery.reshape(row_count, head_cols), dpair_sum], axis=1
        ).astype(jnp.bfloat16)
        grad_qkv_now = dot_rows(inputs_full, dqkv_low)
        grad_list.append(dhidden_one + spread_sum(dot_cols(dqkv_low, qkv_full)))
        micro_grads = (grad_qkv_now, grad_attn_now, grad_up_now, grad_down_now)
        local_grads = tuple(
            (left_val + right_val for left_val, right_val in zip(local_grads, micro_grads))
        )
    final_set = reduce_weights(local_grads, head_cols)
    lead_mask = (lax.axis_index("dp") == 0).astype(jnp.float32)
    sum_gain1, sum_bias1, sum_gain2, sum_bias2, sum_cls_in, sum_pool, sum_mid, sum_top = lax.psum(
        (
            gain_one,
            bias_one,
            gain_two,
            bias_two,
            grad_cls_in,
            grad_pool,
            grad_mid * lead_mask,
            grad_top * lead_mask,
        ),
        ("dp", "rows"),
    )
    return (
        jnp.stack(out_list)[:, None],
        jnp.stack(loss_list)[:, None],
        jnp.stack(grad_list)[:, None],
        final_set[0],
        final_set[1],
        final_set[2],
        final_set[3],
        final_set[4],
        final_set[5],
        sum_gain1,
        sum_bias1,
        sum_gain2,
        sum_bias2,
        sum_cls_in,
        sum_pool,
        sum_mid,
        sum_top,
    )


def dot_at(left, right, contract):
    return lax.dot_general(
        left, right, (contract, ((), ())), preferred_element_type=jnp.float32
    )


NN = ((1,), (0,))
NT = ((1,), (1,))
TN = ((0,), (0,))


def wide(ref):
    return jnp.concatenate([ref[block] for block in range(ref.shape[0])], axis=1)


def attend_kernel(q_ref, k_ref, v_ref, o_ref, low_ref, p_ref, inv_ref):
    keys = wide(k_ref)
    values = wide(v_ref)
    for block in range(q_ref.shape[0]):
        query = q_ref[block]
        scores = dot_at(keys, query, TN) * 0.125
        exps = jnp.exp(scores - jnp.max(scores, axis=0, keepdims=True))
        inverse = 1.0 / jnp.sum(exps, axis=0, keepdims=True)
        low = exps.astype(jnp.bfloat16)
        p_ref[0, block] = low
        inv_ref[0, block] = inverse
        out = dot_at(values, low, NN) * inverse
        o_ref[block] = out
        low_ref[block] = out.astype(jnp.bfloat16)


def attend(qkv):
    blocks, _, width = qkv.shape
    heads = qkv.shape[1] // 192

    def part(offset):
        return pl.BlockSpec((blocks, 64, width), lambda h: (0, h + offset * heads, 0))

    total = blocks * width
    return pl.pallas_call(
        attend_kernel,
        grid=(heads,),
        out_shape=[
            jax.ShapeDtypeStruct((blocks, 64 * heads, width), jnp.float32),
            jax.ShapeDtypeStruct((blocks, 64 * heads, width), jnp.bfloat16),
            jax.ShapeDtypeStruct((heads, blocks, total, width), jnp.bfloat16),
            jax.ShapeDtypeStruct((heads, blocks, 1, width), jnp.float32),
        ],
        in_specs=[part(0), part(1), part(2)],
        out_specs=[
            part(0),
            part(0),
            pl.BlockSpec((1, blocks, total, width), lambda h: (h, 0, 0, 0)),
            pl.BlockSpec((1, blocks, 1, width), lambda h: (h, 0, 0, 0)),
        ],
        compiler_params=pltpu.CompilerParams(vmem_limit_bytes=VMEM_GRANT),
    )(qkv, qkv, qkv)


def attend_back_kernel(q_ref, k_ref, v_ref, d_ref, o_ref, p_ref, inv_ref, dq_ref, dk_ref, dv_ref):
    keys = wide(k_ref)
    values = wide(v_ref)
    width = q_ref.shape[2]
    dkeys = jnp.zeros(keys.shape, jnp.float32)
    dvalues = jnp.zeros(keys.shape, jnp.float32)
    for block in range(q_ref.shape[0]):
        query = q_ref[block]
        grad = d_ref[block].astype(jnp.float32)
        inverse = inv_ref[0, block]
        delta = jnp.sum(grad * o_ref[block], axis=0, keepdims=True) * inverse
        scaled = (grad * inverse).astype(jnp.bfloat16)
        low = p_ref[0, block]
        dprobs = dot_at(values, scaled, TN)
        dscores = (low.astype(jnp.float32) * (dprobs - delta)).astype(jnp.bfloat16)
        dq_ref[block] = (dot_at(keys, dscores, NN) * 0.125).astype(jnp.bfloat16)
        dkeys = dkeys + dot_at(query, dscores, NT)
        dvalues = dvalues + dot_at(scaled, low, NT)
    for block in range(q_ref.shape[0]):
        span = slice(block * width, (block + 1) * width)
        dk_ref[block] = (dkeys[:, span] * 0.125).astype(jnp.bfloat16)
        dv_ref[block] = dvalues[:, span].astype(jnp.bfloat16)


def attend_back(qkv, grad, out, probs, inverse):
    blocks, _, width = qkv.shape
    heads = qkv.shape[1] // 192

    def part(offset):
        return pl.BlockSpec((blocks, 64, width), lambda h: (0, h + offset * heads, 0))

    total = blocks * width
    piece = jax.ShapeDtypeStruct((blocks, 64 * heads, width), jnp.bfloat16)
    return pl.pallas_call(
        attend_back_kernel,
        grid=(heads,),
        out_shape=[piece, piece, piece],
        in_specs=[
            part(0),
            part(1),
            part(2),
            part(0),
            part(0),
            pl.BlockSpec((1, blocks, total, width), lambda h: (h, 0, 0, 0)),
            pl.BlockSpec((1, blocks, 1, width), lambda h: (h, 0, 0, 0)),
        ],
        out_specs=[part(0), part(0), part(0)],
        compiler_params=pltpu.CompilerParams(vmem_limit_bytes=VMEM_GRANT),
    )(qkv, qkv, qkv, grad, out, probs, inverse)


def pool_exchange(part):
    return plane_swap((jnp.broadcast_to(part[None], (4,) + part.shape),), 3)[0]


def layer_norm_rows(hidden, gain_vec, shift_vec):
    average = jnp.mean(hidden, axis=1, keepdims=True)
    spread = jnp.mean(hidden * hidden, axis=1, keepdims=True) - average * average
    inv_std = lax.rsqrt(spread + eps_norm)
    centred = (hidden - average) * inv_std
    return (centred * gain_vec + shift_vec, centred, inv_std)


def layer_norm_back(upstream, centred, inv_std, gain_vec):
    scaled = upstream * gain_vec
    return inv_std * (
        scaled
        - jnp.mean(scaled, axis=1, keepdims=True)
        - centred * jnp.mean(scaled * centred, axis=1, keepdims=True)
    )


def quad_body(
    tokens,
    cotangent,
    labels,
    q_weight,
    k_weight,
    v_weight,
    out_weight,
    up_weight,
    down_weight,
    ln1_gain,
    ln1_bias,
    ln2_gain,
    ln2_bias,
    cls_in,
    pool_query,
    cls_mid,
    cls_out,
):
    low = jnp.bfloat16
    rows_here = tokens.shape[2]
    pool_dim = CLS_D // POOL_HEADS
    pool_root = math.sqrt(pool_dim)
    qkv_shard = jnp.concatenate([q_weight.T, k_weight.T, v_weight.T], axis=0)
    norm_shard = jnp.pad(
        jnp.stack([ln1_gain, ln1_bias, ln2_gain, ln2_bias]), ((0, 4), (0, 64))
    )
    x4, cot4, norms4, cls4, w_qkv, w_out, w_up, w_down = gather_all(
        (tokens[:, 0], cotangent[:, 0]),
        (norm_shard, cls_in),
        (qkv_shard, out_weight, up_weight.T, down_weight),
    )
    inputs = jnp.transpose(x4, (1, 0, 2)).reshape(rows_here, D)
    cot = jnp.transpose(cot4, (1, 0, 2)).reshape(rows_here, D)
    norms = jnp.transpose(norms4[:, :4, :192], (1, 0, 2)).reshape(4, D)
    gain_one, bias_one, gain_two, bias_two = (norms[i][None] for i in range(4))
    cls_full = cls4.reshape(D, CLS_D)
    w_qkv, w_out, w_up, w_down = (w.reshape(-1, D) for w in (w_qkv, w_out, w_up, w_down))

    qkv = dot_at(w_qkv, inputs, NT).astype(low).reshape(4, 576, rows_here)
    qkv = plane_swap((qkv,), 2)[0]
    attended, attended_heads, probs, inverse = attend(qkv)
    attended_low = plane_swap((attended_heads,), 4)[0].reshape(D, rows_here)
    branch = dot_at(attended_low, w_out, TN)
    normed, centred_one, inv_one = layer_norm_rows(
        inputs.astype(jnp.float32) + branch, gain_one, bias_one
    )
    normed_low = normed.astype(low)
    up_pre = dot_at(w_up, normed_low, NT)
    activated, gelu_back = jax.vjp(exact_gelu, up_pre)
    activated_low = activated.astype(low)
    down_out = dot_at(activated_low, w_down, TN)
    outputs, centred_two, inv_two = layer_norm_rows(normed + down_out, gain_two, bias_two)
    outputs_low = outputs.astype(low)
    cls_proj = jnp.dot(outputs_low, cls_full, preferred_element_type=jnp.float32)
    pool_heads = cls_proj.reshape(rows_here, POOL_HEADS, pool_dim)
    pool_scores = jnp.einsum("lpd,pd->lp", pool_heads, pool_query, precision=highest) / pool_root
    local_top = jnp.max(pool_scores, axis=0)
    pool_exp = jnp.exp(pool_scores - local_top)
    stats = jnp.stack(
        [
            jnp.repeat(local_top, pool_dim),
            jnp.repeat(jnp.sum(pool_exp, axis=0), pool_dim),
            jnp.einsum("lp,lpd->pd", pool_exp, pool_heads, precision=highest).reshape(CLS_D),
        ]
    )
    stats = pool_exchange(jnp.pad(stats, ((0, 5), (0, 0))))
    joint_top = jnp.max(stats[:, 0], axis=0)
    rescale = jnp.exp(stats[:, 0] - joint_top)
    joint_total = jnp.sum(stats[:, 1] * rescale, axis=0)
    pooled_row = (jnp.sum(stats[:, 2] * rescale, axis=0) / joint_total)[None]
    pooled = pooled_row.reshape(POOL_HEADS, pool_dim)
    pool_weights = jnp.exp(pool_scores - joint_top[::pool_dim]) / joint_total[::pool_dim]
    hidden_cls = jnp.tanh(jnp.dot(pooled_row, cls_mid, precision=highest))
    logits = jnp.dot(hidden_cls, cls_out, precision=highest)[0]
    col = lax.axis_index("cols")
    label = lax.dynamic_index_in_dim(labels[:, 0], col, 0, False)
    target_hit = lax.iota(jnp.int32, CLASSES) == label
    loss = jax.nn.logsumexp(logits) - jnp.sum(jnp.where(target_hit, logits, 0.0))
    dlogits = jax.nn.softmax(logits) - target_hit.astype(jnp.float32)
    grad_top = hidden_cls[0][:, None] * dlogits[None, :]
    dhidden = jnp.dot(cls_out, dlogits, precision=highest)
    dpre_tanh = dhidden * (1.0 - hidden_cls[0] * hidden_cls[0])
    grad_mid = pooled_row[0][:, None] * dpre_tanh[None, :]
    dpooled = jnp.dot(cls_mid, dpre_tanh, precision=highest).reshape(POOL_HEADS, pool_dim)
    dweights = jnp.einsum("lpd,pd->lp", pool_heads, dpooled, precision=highest)
    dpool_scores = pool_weights * (dweights - jnp.sum(pooled * dpooled, axis=1))
    dheads = (
        pool_weights[:, :, None] * dpooled[None]
        + dpool_scores[:, :, None] * (pool_query / pool_root)[None]
    )
    grad_pool = jnp.einsum("lp,lpd->pd", dpool_scores, pool_heads, precision=highest) / pool_root
    dproj_low = dheads.reshape(rows_here, CLS_D).astype(low)
    grad_cls_in = dot_rows(outputs_low, dproj_low)
    upstream = cot.astype(jnp.float32) + dot_cols(dproj_low, cls_full)
    sums = [jnp.sum(upstream * centred_two, axis=0), jnp.sum(upstream, axis=0)]
    dhidden_two = layer_norm_back(upstream, centred_two, inv_two, gain_two)
    ddown = dhidden_two.astype(low)
    g_down = dot_at(activated_low, ddown, NN).astype(low)
    dup = gelu_back(dot_at(w_down, ddown, NT))[0].astype(low)
    g_up = dot_at(dup, normed_low, NN).astype(low)
    dnormed = dhidden_two + dot_at(dup, w_up, TN)
    sums += [jnp.sum(dnormed * centred_one, axis=0), jnp.sum(dnormed, axis=0)]
    dhidden_one = layer_norm_back(dnormed, centred_one, inv_one, gain_one)
    dbranch = dhidden_one.astype(low)
    g_out = dot_at(attended_low, dbranch, NN).astype(low)
    dattended = dot_at(w_out, dbranch, NT).astype(low).reshape(4, 192, rows_here)
    dattended = plane_swap((dattended,), 5)[0]
    dqkv = jnp.concatenate(attend_back(qkv, dattended, attended, probs, inverse), axis=1)
    dqkv = plane_swap((dqkv,), 6)[0].reshape(4 * 576, rows_here)
    g_qkv = dot_at(dqkv, inputs, NN).astype(low)
    grad_inputs = dhidden_one + dot_at(dqkv, w_qkv, TN)

    lead = (lax.axis_index("dp") == 0).astype(jnp.float32)
    slot = lax.axis_index("rows") * 4 + col
    loss_row = jnp.where(lax.iota(jnp.int32, CLS_D) == slot, loss * lead, 0.0)
    packed = jnp.concatenate(
        [
            grad_cls_in,
            jnp.stack(sums).reshape(4 * D // CLS_D, CLS_D),
            grad_mid * lead,
            grad_top.T * lead,
            grad_pool.reshape(1, CLS_D),
            loss_row[None],
        ],
        axis=0,
    )
    packed = lax.psum(packed, ("dp", "rows", "cols"))
    sum_cls_in = lax.dynamic_slice_in_dim(packed[:D], col * 192, 192, 0)
    norm_sums = lax.dynamic_slice_in_dim(packed[D : D + 24].reshape(4, D), col * 192, 192, 1)
    at = D + 24
    sum_mid = packed[at : at + CLS_D]
    sum_top = packed[at + CLS_D : at + CLS_D + CLASSES].T
    sum_pool = packed[at + CLS_D + CLASSES].reshape(POOL_HEADS, pool_dim)
    losses = lax.dynamic_slice_in_dim(packed[at + CLS_D + CLASSES + 1], (slot - col), 4, 0)

    def features_out(value):
        blocks = jnp.transpose(value.reshape(rows_here, 4, 192), (1, 0, 2))
        return blocks

    out_blocks, grad_blocks, r_qkv, r_out, r_up, r_down = reduce_all(
        (features_out(outputs_low), features_out(grad_inputs.astype(low))),
        (g_qkv, g_out, g_up, g_down),
    )
    wide_ = jnp.float32
    return (
        out_blocks[:, None],
        losses[:, None],
        grad_blocks.astype(wide_)[:, None],
        r_qkv[:192].T.astype(wide_),
        r_qkv[192:384].T.astype(wide_),
        r_qkv[384:].T.astype(wide_),
        r_out.astype(wide_),
        r_up.T.astype(wide_),
        r_down.astype(wide_),
        norm_sums[2],
        norm_sums[3],
        norm_sums[0],
        norm_sums[1],
        sum_cls_in,
        sum_pool,
        sum_mid,
        sum_top,
    )


def add_rows(dst, source, lead, start, count):
    def one(block, unused):
        spot = dst.at[lead(block), pl.ds(start, count)]
        total = spot[...].astype(jnp.float32) + source(block)[...].astype(jnp.float32)
        spot[...] = total.astype(jnp.bfloat16)
        return unused

    lax.fori_loop(0, 4, one, 0)


def reduce_kernel(number, counts):
    segs = len(counts)

    def kernel(*refs):
        swap_in, grads = refs[:number], refs[number : number + segs]
        rest = refs[number + segs :]
        swap_out, outs = rest[:number], rest[number : number + segs]
        rest = rest[number + segs :]
        acc, twin_buf, first_a, first_b, next_a, next_b, zbuf, final = (
            rest[i * segs : (i + 1) * segs] for i in range(8)
        )
        ssend, srecv, send_sem, recv_sem, local_sem = rest[8 * segs :]
        p, r, c = position()
        px, py, diag = plane_x(p), plane_y(p), 3 - p
        x_dev, y_dev, twin = (px, r, c), (py, r, c), (p, 1 - r, c)
        greet([(p, r, (c + k) % 4) for k in range(1, 4)] + [x_dev, y_dev, twin])
        sent, locals_ = [], []

        def keep(src, dst, index):
            copy = pltpu.make_async_copy(src, dst, local_sem.at[index])
            copy.start()
            return copy

        def send(g, src, dst, slot, device):
            copy = remote(src, dst, send_sem.at[g, slot], recv_sem.at[g, slot], device)
            copy.start()
            sent.append(copy)

        def wait(g, view, slot):
            remote(view, view, send_sem.at[g, slot], recv_sem.at[g, slot], twin).wait_recv()

        lanes = pl.ds(pl.multiple_of(r * HALF, HALF), HALF)
        other_lanes = pl.ds(pl.multiple_of((1 - r) * HALF, HALF), HALF)
        mine = []
        for g in range(segs):
            send(g, grads[g].at[:, :, other_lanes], twin_buf[g], 0, twin)
            mine.append(keep(grads[g].at[:, :, lanes], acc[g], g))
        for index in range(number):
            for k in range(1, 4):
                peer = (c + k) % 4
                copy = remote(
                    swap_in[index].at[peer],
                    swap_out[index].at[c],
                    ssend.at[index, k - 1],
                    srecv.at[index, 3 - k],
                    (p, r, peer),
                )
                copy.start()
                sent.append(copy)
            locals_.append(keep(swap_in[index].at[c], swap_out[index].at[c], segs + index))

        def span(g, quarter, part=None):
            count = counts[g] // 4
            halves = split_rows(count)
            start = pl.multiple_of(quarter * count, 16)
            if part is None:
                return start, count
            return pl.multiple_of(start + part * halves[0], 16), halves[part]

        def cut(g, quarter, part=None):
            return pl.ds(*span(g, quarter, part))

        def same(block):
            return block

        def pair(g):
            mine[g].wait()
            wait(g, twin_buf[g], 0)

            def one(index, unused):
                block, step = index % 4, index // 4
                part = pl.ds(pl.multiple_of(step * 48, 16), 48)
                total = acc[g][block, part].astype(jnp.float32)
                total = total + twin_buf[g][block, part].astype(jnp.float32)
                acc[g][block, part] = total.astype(jnp.bfloat16)
                return unused

            lax.fori_loop(0, 4 * (counts[g] // 48), one, 0)
            send(g, acc[g].at[:, cut(g, diag, 0)], first_a[g].at[1], 1, x_dev)
            send(g, acc[g].at[:, cut(g, diag, 1)], first_b[g].at[1], 2, y_dev)
            send(g, acc[g].at[:, cut(g, px, 0)], first_a[g].at[0], 3, x_dev)
            send(g, acc[g].at[:, cut(g, py, 1)], first_b[g].at[0], 4, y_dev)

        def second(g):
            wait(g, first_a[g].at[1], 1)
            add_rows(acc[g], lambda b: first_a[g].at[1, b], same, *span(g, py, 0))
            send(g, acc[g].at[:, cut(g, py, 0)], next_a[g], 5, y_dev)
            wait(g, first_b[g].at[1], 2)
            add_rows(acc[g], lambda b: first_b[g].at[1, b], same, *span(g, px, 1))
            send(g, acc[g].at[:, cut(g, px, 1)], next_b[g], 6, x_dev)
            wait(g, first_a[g].at[0], 3)
            add_rows(acc[g], lambda b: first_a[g].at[0, b], same, *span(g, p, 0))
            wait(g, first_b[g].at[0], 4)
            add_rows(acc[g], lambda b: first_b[g].at[0, b], same, *span(g, p, 1))

        def third(g):
            wait(g, next_a[g], 5)
            add_rows(acc[g], lambda b: next_a[g].at[b], same, *span(g, p, 0))
            wait(g, next_b[g], 6)
            add_rows(acc[g], lambda b: next_b[g].at[b], same, *span(g, p, 1))
            for k in (2, 1, 3):
                peer = (c + k) % 4
                copy = remote(
                    acc[g].at[peer, cut(g, p)],
                    zbuf[g].at[3 - k],
                    send_sem.at[g, 6 + k],
                    recv_sem.at[g, 10 - k],
                    (p, r, peer),
                )
                copy.start()
                sent.append(copy)

        def fourth(g):
            total = acc[g][c, cut(g, p)].astype(jnp.float32)
            for k in range(3):
                wait(g, zbuf[g].at[k], 7 + k)
                total = total + zbuf[g][k].astype(jnp.float32)
            final[g][cut(g, p)] = total.astype(jnp.bfloat16)
            own = final[g].at[cut(g, p)]
            send(g, own, own, 10, x_dev)
            send(g, own, own, 11, y_dev)

        def fifth(g):
            wait(g, final[g].at[cut(g, px)], 10)
            view = final[g].at[cut(g, px, 0)]
            send(g, view, view, 12, y_dev)
            wait(g, final[g].at[cut(g, py)], 11)
            view = final[g].at[cut(g, py, 1)]
            send(g, view, view, 13, x_dev)

        def sixth(g):
            wait(g, final[g].at[cut(g, diag, 0)], 12)
            wait(g, final[g].at[cut(g, diag, 1)], 13)
            locals_.append(keep(final[g], outs[g], segs + number + g))

        stages = (pair, second, third, fourth, fifth, sixth)
        for step in range(segs + len(stages) - 1):
            for index, stage in enumerate(stages):
                if 0 <= step - index < segs:
                    stage(step - index)
        for index in range(number):
            for k in range(1, 4):
                view = swap_out[index].at[(c + k) % 4]
                remote(view, view, ssend.at[index, k - 1], srecv.at[index, k - 1], twin).wait_recv()
        for copy in sent:
            copy.wait_send()
        for copy in locals_:
            copy.wait()

    return kernel


def reduce_call(swaps, grads, ident):
    low = jnp.bfloat16
    grads = [g.reshape(4, -1, 2 * HALF) for g in grads]
    counts = [g.shape[1] for g in grads]
    halves = [split_rows(n // 4) for n in counts]
    scratch = [pltpu.VMEM((4, n, HALF), low) for n in counts] * 2
    scratch += [pltpu.VMEM((2, 4, h[0], HALF), low) for h in halves]
    scratch += [pltpu.VMEM((2, 4, h[1], HALF), low) for h in halves]
    scratch += [pltpu.VMEM((4, h[0], HALF), low) for h in halves]
    scratch += [pltpu.VMEM((4, h[1], HALF), low) for h in halves]
    scratch += [pltpu.VMEM((3, n // 4, HALF), low) for n in counts]
    scratch += [pltpu.VMEM((n, HALF), low) for n in counts]
    dma = pltpu.SemaphoreType.DMA
    number, segs = len(swaps), len(counts)
    scratch += [
        dma((max(number, 1), 3)),
        dma((max(number, 1), 3)),
        dma((segs, 14)),
        dma((segs, 14)),
        dma((2 * segs + number,)),
    ]
    outs = [jax.ShapeDtypeStruct(a.shape, a.dtype) for a in swaps]
    outs += [jax.ShapeDtypeStruct((n, HALF), low) for n in counts]
    return comm_call(reduce_kernel(number, counts), (*swaps, *grads), outs, scratch, ident)


def reduce_all(swaps, grads):
    g_qkv, g_out, g_up, g_down = grads
    moved_out, moved_in, r_down, r_up, r_out, r_qkv = reduce_call(
        swaps, (g_down, g_up, g_out, g_qkv), 7
    )
    return (moved_out, moved_in, r_qkv, r_out, r_up, r_down)


def solution(mesh):
    placed = (
        P(None, "rows", "dp", "cols"),
        P(None, "rows", "dp", "cols"),
        P(None, "rows"),
        P("rows", "cols"),
        P("rows", "cols"),
        P("rows", "cols"),
        P("cols", "rows"),
        P("rows", "cols"),
        P("cols", "rows"),
        P("cols"),
        P("cols"),
        P("cols"),
        P("cols"),
        P("cols", None),
        P(),
        P(),
        P(),
    )
    even = dict(mesh.shape) == {"dp": 4, "rows": 2, "cols": 4}
    return jax.shard_map(
        quad_body if even else body,
        mesh=mesh,
        in_specs=placed,
        out_specs=(
            P(None, "rows", "dp", "cols"),
            P(None, "rows"),
            P(None, "rows", "dp", "cols"),
            P("rows", "cols"),
            P("rows", "cols"),
            P("rows", "cols"),
            P("cols", "rows"),
            P("rows", "cols"),
            P("cols", "rows"),
            P("cols"),
            P("cols"),
            P("cols"),
            P("cols"),
            P("cols", None),
            P(),
            P(),
            P(),
        ),
        check_vma=False,
    )
```
